128 devices in a mesh: seq: 16 (over z_hi, y, core), head: 8 (over x, z_lo).
Axes of the slice: x: 4, y: 4, z: 4 (z_hi: 2, z_lo: 2; z = z_hi * 2 + z_lo), core: 2. Of those that a mesh axis runs over, the one named last changes fastest.
Arguments:
- latent: bfloat16 [16, 1024, 2048], P('seq', None, 'head'), may hold values from -6 to 6
- modulation: float32 [9, 2048], replicated, may hold values from -3 to 3
- spatial_qkv: bfloat16 [3, 2048, 2048], P(None, None, 'head')
- spatial_out: bfloat16 [2048, 2048], P('head'), may hold values from -0.125 to 0.125
- temporal_qkv: bfloat16 [3, 2048, 2048], P(None, None, 'head')
- temporal_out: bfloat16 [2048, 2048], P('head'), may hold values from -0.125 to 0.125
- hidden_weight: bfloat16 [2048, 8192], P(None, 'head'), may hold values from -0.125 to 0.125
- output_weight: bfloat16 [8192, 2048], P('head'), may hold values from -0.0625 to 0.0625
Outputs:
- block_out: bfloat16 [16, 1024, 2048], P(None, 'seq', 'head')
The draws below stay inside these ranges and needn't reach their ends.
All inputs are finite; a program needn't handle non-finite values.
Results may differ from the reference program's by a relative error of at most 0.009.
Values may be sent and summed in bfloat16 or wider, within the bound.
A program may use at most 128 MiB of HBM per device.

```python
import jax
import jax.numpy as jnp
from jax import lax

D = 2048
HEADS = 32
FF = 8192
P_SIZE = 1024
HD = 64
FRAMES = 16


def projection_draw(key, salt):
    key = jax.random.fold_in(key, salt)
    first, second, third = jax.random.split(key, 3)
    spread = D ** (-0.5)
    query = jax.random.normal(first, (D, D), jnp.float32) * spread
    keys = jax.random.normal(second, (D, D), jnp.float32) * spread
    values = jax.random.normal(third, (D, D), jnp.float32) * spread
    return jnp.stack([query, keys, values]).astype(jnp.bfloat16)


def draw_spatial_qkv(key, part):
    return projection_draw(key, 11)


def draw_temporal_qkv(key, part):
    return projection_draw(key, 23)


def level_of(rng, extent, cuts, least, high):
    factor_of = 1.0
    for dim, parts in cuts:
        draws = jax.random.uniform(jax.random.fold_in(jax.random.fold_in(rng, 6), dim), (parts,), jnp.float32, least / len(cuts), high / len(cuts))
        factor_of = factor_of * jnp.repeat(jnp.exp(draws), extent[dim] // parts).reshape((-1,) + (1,) * (len(extent) - 1 - dim))
    return factor_of


def normal_values(stream_key, shape, scale, most, cuts=(), kind=jnp.bfloat16):
    drawn = jax.random.normal(stream_key, shape, jnp.float32) * scale
    if len(cuts) > 0:
        drawn = level_of(stream_key, shape, cuts, -0.22, 0.18) * drawn
    return jnp.clip(drawn, min=-most, max=most).astype(kind)


def setup_inputs(seed: int = 0) -> dict:
    arg_keys = jax.random.split(jax.random.key(seed), 9)
    return {
        "latent": normal_values(arg_keys[0], (FRAMES, P_SIZE, D), 1.0, 6.0, ((0, 16), (2, 8))),
        "modulation": normal_values(arg_keys[1], (9, D), 0.5, 3.0, (), jnp.float32),
        "spatial_qkv": draw_spatial_qkv(jax.random.fold_in(arg_keys[8], 71), 0),
        "spatial_out": normal_values(arg_keys[3], (D, D), D ** -0.5, 0.125, ((0, 8),)),
        "temporal_qkv": draw_temporal_qkv(jax.random.fold_in(arg_keys[8], 71), 0),
        "temporal_out": normal_values(arg_keys[5], (D, D), D ** -0.5, 0.125, ((0, 8),)),
        "hidden_weight": normal_values(arg_keys[6], (D, FF), D ** -0.5, 0.125, ((1, 8),)),
        "output_weight": normal_values(arg_keys[7], (FF, D), FF ** -0.5, 0.0625, ((0, 8),)),
    }


def layer_norm(values):
    average = lax.optimization_barrier(jnp.mean(values, axis=-1, keepdims=True))
    centred = values - average
    variance = lax.optimization_barrier(jnp.mean(centred * centred, axis=-1, keepdims=True))
    return centred * lax.rsqrt(variance + 1e-06)

def modulate(stream, modulation, offset):
    normed = layer_norm(stream.astype(jnp.float32))
    return (normed * (1.0 + modulation[offset + 1]) + modulation[offset]).astype(jnp.bfloat16)

def attend(query, keys, values):
    scores = jnp.einsum('glhd,gmhd->ghlm', query.astype(jnp.float32), keys.astype(jnp.float32)) * HD ** (-0.5)
    attn_weights = jax.nn.softmax(scores, axis=-1).astype(jnp.bfloat16)
    return jnp.einsum('ghlm,gmhd->glhd', attn_weights.astype(jnp.float32), values.astype(jnp.float32)).astype(jnp.bfloat16)

def project_three(normed, weights):
    return [jnp.dot(normed, weights[member], preferred_element_type=jnp.float32).astype(jnp.bfloat16) for member in range(3)]

def reference(latent, modulation, spatial_qkv, spatial_out, temporal_qkv, temporal_out, hidden_weight, output_weight):
    frames = latent.shape[0]
    patches = latent.shape[1]

    def split_heads(tensor):
        return tensor.reshape(frames, patches, HEADS, HD)
    normed = modulate(latent, modulation, 0)
    query, keys, values = [split_heads(member) for member in project_three(normed, spatial_qkv)]
    spatial = lax.map(lambda triple: attend(triple[0][None], triple[1][None], triple[2][None])[0], (query, keys, values))
    spatial = spatial.reshape(frames, patches, D)
    branch = jnp.dot(spatial, spatial_out, preferred_element_type=jnp.float32)
    stream_one = (latent.astype(jnp.float32) + modulation[2] * branch).astype(jnp.bfloat16)
    normed = modulate(stream_one, modulation, 3)
    query, keys, values = [jnp.transpose(split_heads(member), (1, 0, 2, 3)) for member in project_three(normed, temporal_qkv)]
    temporal = jnp.transpose(attend(query, keys, values), (1, 0, 2, 3)).reshape(frames, patches, D)
    branch = jnp.dot(temporal, temporal_out, preferred_element_type=jnp.float32)
    stream_two = (stream_one.astype(jnp.float32) + modulation[5] * branch).astype(jnp.bfloat16)
    normed = modulate(stream_two, modulation, 6)
    hidden = jax.nn.gelu(jnp.dot(normed, hidden_weight, preferred_element_type=jnp.float32), approximate=True).astype(jnp.bfloat16)
    branch = jnp.dot(hidden, output_weight, preferred_element_type=jnp.float32)
    return (stream_two.astype(jnp.float32) + modulation[8] * branch).astype(jnp.bfloat16)
```

```python
import functools

import jax
import jax.numpy as jnp
from jax import lax
from jax.experimental import pallas as pl
from jax.experimental.pallas import tpu as pltpu
from jax.sharding import PartitionSpec as P

MESH = pl.DeviceIdType.MESH
BF = jnp.bfloat16
F32 = jnp.float32
T = 1024
D = 2048
B = 256
VM = pltpu.VMEM
ANY = pl.BlockSpec(memory_space=pl.ANY)
INV = pl.BlockSpec(memory_space=pltpu.VMEM)


def rc(src, dst, ss, rs, dev):
    return pltpu.make_async_remote_copy(
        src_ref=src, dst_ref=dst, send_sem=ss, recv_sem=rs, device_id=dev, device_id_type=MESH
    )


class Place:
    def __init__(self):
        s, h = lax.axis_index("seq"), lax.axis_index("head")
        self.c, self.y, self.zh = lax.rem(s, 2), lax.rem(lax.div(s, 2), 4), lax.div(s, 8)
        self.x, self.zl = lax.div(h, 2), lax.rem(h, 2)
        self.z = self.zh * 2 + self.zl
        self.o = 1 - self.c
        self.row = (self.zh * 4 + self.y) * 2 + self.zl
        self.xr, self.xl, self.xf = [lax.rem(self.x + k, 4) for k in (1, 3, 2)]
        self.R = self.dev(self.xr, self.z, self.c)
        self.L = self.dev(self.xl, self.z, self.c)
        self.D = self.dev(self.x, self.z, self.o)
        self.U = self.dev(self.x, lax.rem(self.z + 1, 4), self.c)
        self.N = self.dev(self.x, lax.rem(self.z + 3, 4), self.c)
        self.S = ((self.zh * 4 + self.y) * 2 + self.o, self.x * 2 + 1 - self.zl)

    def dev(self, x, z, c):
        return ((lax.div(z, 2) * 4 + self.y) * 2 + c, x * 2 + lax.rem(z, 2))

    def row_dev(self, row):
        return (lax.div(row, 2) * 2 + self.c, self.x * 2 + lax.rem(row, 2))


def greet(devices):
    barrier = pltpu.get_barrier_semaphore()
    for device in devices:
        pl.semaphore_signal(barrier, inc=1, device_id=device, device_id_type=MESH)
    pl.semaphore_wait(barrier, len(devices))


def blk(x, c, width=B, off=0):
    return pl.ds(pl.multiple_of((x * 2 + c) * B + off, 128), width)


class Gather:
    KINDS = 9

    def __init__(self, p, full, rows, ss, rs):
        self.p, self.full, self.rows, self.ss, self.rs = p, full, rows, ss, rs
        x, c, o = p.x, p.c, p.o
        H = 128
        self.sent = [
            (blk(x, c), p.R), (blk(x, c), p.L), (blk(x, c), p.D),
            (blk(p.xl, c, H), p.R), (blk(p.xr, c, H, H), p.L),
            (blk(p.xl, c), p.D), (blk(p.xr, c), p.D),
            (blk(p.xf, c, H), p.D), (blk(p.xf, c, H, H), p.D),
        ]
        self.landed = [
            blk(p.xl, c), blk(p.xr, c), blk(x, o),
            blk(p.xf, c, H), blk(p.xf, c, H, H),
            blk(p.xl, o), blk(p.xr, o),
            blk(p.xf, o, H), blk(p.xf, o, H, H),
        ]

    def out(self, k, t):
        cols, dev = self.sent[k]
        ref = self.full.at[(*self.rows(t), cols)]
        return rc(ref, ref, self.ss.at[k, t], self.rs.at[k, t], dev)

    def got(self, k, t):
        ref = self.full.at[(*self.rows(t), self.landed[k])]
        rc(ref, ref, self.ss.at[k, t], self.rs.at[k, t], self.sent[k][1]).wait_recv()

    def own(self, t):
        for k in (0, 1, 2):
            self.out(k, t).start()

    def relay(self, t):
        self.got(0, t)
        self.out(3, t).start()
        self.out(5, t).start()
        self.got(1, t)
        self.out(4, t).start()
        self.out(6, t).start()

    def far(self, t):
        self.got(3, t)
        self.out(7, t).start()
        self.got(4, t)
        self.out(8, t).start()

    def arrive(self, t):
        for k in (2, 5, 6, 7, 8):
            self.got(k, t)

    def drain(self, t):
        for k in range(9):
            self.out(k, t).wait_send()


class Reduce:
    def __init__(self, p, ch, act, half, w, part, fs, fr, ns, nr, ss, rs):
        self.p, self.ch, self.act, self.half, self.w, self.part = p, ch, act, half, w, part
        self.fs, self.fr, self.ns, self.nr, self.ss, self.rs = fs, fr, ns, nr, ss, rs

    def r(self, t):
        return pl.ds(pl.multiple_of(t * self.ch, self.ch), self.ch)

    def copy(self, k, t):
        p, r = self.p, self.r(t)
        if k == 0:
            src, dst, dev = self.act.at[r, 0 : self.half], self.act.at[r, self.half : 2 * self.half], p.D
        elif k in (1, 2):
            src, dst, dev = self.fs.at[k - 1, r], self.fr.at[k - 1, r], (p.R, p.L)[k - 1]
        else:
            src, dst, dev = self.ns.at[k - 3, r], self.nr.at[k - 3, r], (p.R, p.L)[k - 3]
        return rc(src, dst, self.ss.at[k, t], self.rs.at[k, t], dev)

    def share(self, t):
        self.copy(0, t).start()

    def project(self, t):
        r = self.r(t)
        self.copy(0, t).wait_recv()
        out = jnp.dot(self.act[r, :], self.w[...], preferred_element_type=F32)
        self.fs[0, r] = out[:, 512:640].astype(BF)
        self.fs[1, r] = out[:, 640:768].astype(BF)
        self.copy(1, t).start()
        self.copy(2, t).start()
        self.part[r, 0:512] = out[:, 0:512]
        self.part[r, 512:768] = out[:, 768:1024]

    def near(self, t):
        r = self.r(t)
        self.copy(1, t).wait_recv()
        self.ns[0, r, 0:128] = (self.part[r, 256:384] + self.fr[0, r].astype(F32)).astype(BF)
        self.ns[0, r, 128:256] = self.part[r, 384:512].astype(BF)
        self.copy(3, t).start()
        self.copy(2, t).wait_recv()
        self.ns[1, r, 0:128] = self.part[r, 512:640].astype(BF)
        self.ns[1, r, 128:256] = (self.part[r, 640:768] + self.fr[1, r].astype(F32)).astype(BF)
        self.copy(4, t).start()

    def total(self, t):
        r = self.r(t)
        self.copy(3, t).wait_recv()
        self.copy(4, t).wait_recv()
        return self.part[r, 0:256] + self.nr[0, r].astype(F32) + self.nr[1, r].astype(F32)

    def drain(self, t):
        for k in range(5):
            self.copy(k, t).wait_send()


def reduce_scratch(nc, width):
    return [
        VM((T, width), BF), VM((width, 1024), BF), VM((T, 768), F32),
        VM((2, T, 128), BF), VM((2, T, 128), BF), VM((2, T, B), BF), VM((2, T, B), BF),
        pltpu.SemaphoreType.DMA((5, nc)), pltpu.SemaphoreType.DMA((5, nc)),
    ]


def normed(values, mod, row):
    v = values.astype(F32)
    v = v - jnp.mean(v, axis=-1, keepdims=True)
    v = v * lax.rsqrt(jnp.mean(v * v, axis=-1, keepdims=True) + 1e-06)
    return (v * (1.0 + mod[row + 1 : row + 2, :]) + mod[row : row + 1, :]).astype(BF)


def stages(n, *steps):
    last = max(lag for lag, _ in steps)

    def body(i, carry):
        for lag, function in steps:
            t = i - lag

            @pl.when((t >= 0) & (t < n))
            def _(t=t, function=function):
                function(t)

        return carry

    lax.fori_loop(0, n + last, body, 0)


def each(n, function):
    def body(i, carry):
        function(i)
        return carry

    lax.fori_loop(0, n, body, 0)


class QKV:
    def __init__(self, p, w, mine, theirs, ss, rs, ls):
        self.p, self.w, self.mine, self.theirs, self.ss, self.rs, self.ls = p, w, mine, theirs, ss, rs, ls

    def pieces(self):
        half = pl.ds(pl.multiple_of(self.p.c * 128, 128), 128)
        for j in range(3):
            yield j, self.ls.at[j], pltpu.make_async_copy(
                self.w.at[j, :, half], self.mine.at[:, j * 128 : j * 128 + 128], self.ls.at[j]
            )

    def sends(self):
        half = pl.ds(pl.multiple_of(self.p.c * 128, 128), 128)
        for j in range(3):
            for d, dev in enumerate((self.p.U, self.p.N)):
                yield rc(
                    self.w.at[j, d * 1024 : d * 1024 + 1024, half],
                    self.theirs.at[d * 1024 : d * 1024 + 1024, j * 128 : j * 128 + 128],
                    self.ss.at[j * 2 + d], self.rs.at[j * 2 + d], dev,
                )

    def start(self):
        for copy in self.sends():
            copy.start()
        for _, _, copy in self.pieces():
            copy.start()

    def wait_mine(self):
        for _, _, copy in self.pieces():
            copy.wait()

    def wait_theirs(self):
        for copy in self.sends():
            copy.wait_recv()

    def drain(self):
        for copy in self.sends():
            copy.wait_send()


class Out:
    def __init__(self, p, w, dst, rows, ss, rs, ls, stage=None):
        self.p, self.w, self.dst, self.rows, self.ss, self.rs, self.ls, self.stage = p, w, dst, rows, ss, rs, ls, stage

    def src(self, g, j):
        half = (self.p.c, self.p.o)[g]
        n = self.rows
        return self.w.at[pl.ds(pl.multiple_of(half * n, n), n), blk(lax.rem(self.p.x + j, 4), self.p.c)]

    def locals(self):
        n = self.rows
        for g in range(2):
            for j in range(4):
                yield pltpu.make_async_copy(
                    self.src(g, j), self.dst.at[2 * g * n : 2 * g * n + n, j * B : j * B + B], self.ls.at[g * 4 + j]
                )

    def sends(self):
        n = self.rows
        for g in range(2):
            for j in range(4):
                if self.stage is None:
                    dst = self.dst.at[2 * g * n + n : 2 * g * n + 2 * n, j * B : j * B + B]
                else:
                    dst = self.stage.at[g * n : g * n + n, j * B : j * B + B]
                yield rc(
                    self.src(g, j), dst,
                    self.ss.at[g * 4 + j], self.rs.at[g * 4 + j], (self.p.U, self.p.N)[g],
                )

    def wait_recv(self):
        for copy in self.sends():
            copy.wait_recv()

    def drain(self):
        for copy in self.sends():
            copy.wait_send()


DMA = pltpu.SemaphoreType.DMA
NC, CH = 8, 128


def flat_rows(t):
    return (pl.ds(pl.multiple_of(t * CH, CH), CH),)


def spatial_in(latent, mod, w, qkv, own, full, nrm, mine, theirs, gs, gr, ws, wr, wl, ls, ss, sr):
    p = Place()
    greet([p.L, p.R, p.D, p.U, p.N, p.S])
    gather = Gather(p, full, flat_rows, gs, gr)
    weights = QKV(p, w, mine, theirs, ws, wr, wl)
    here = blk(p.x, p.c)

    def keep(t):
        r = flat_rows(t)[0]
        return pltpu.make_async_copy(latent.at[0, r, :], full.at[r, here], ls.at[t])

    def swap(t):
        r = flat_rows(t)[0]
        return rc(latent.at[0, r, :], full.at[r, blk(p.x, p.o)], ss.at[t], sr.at[t], p.S)

    def landed(t):
        r = flat_rows(t)[0]
        return rc(latent.at[0, r, :], full.at[r, here], ss.at[t], sr.at[t], p.S)

    @pl.when(p.c == p.zl)
    def _():
        each(NC, lambda t: keep(t).start())

    @pl.when(p.c != p.zl)
    def _():
        each(NC, lambda t: swap(t).start())

    weights.start()

    def first(t):
        @pl.when(p.c == p.zl)
        def _():
            keep(t).wait()

        @pl.when(p.c != p.zl)
        def _():
            landed(t).wait_recv()

        gather.own(t)

    def compute(t):
        gather.arrive(t)
        r = flat_rows(t)[0]
        nrm[r, :] = normed(full[r, :], mod, 0)
        own[r, :] = full[r, here]

        @pl.when(t == 0)
        def _():
            weights.wait_mine()

        qkv[r, 0:384] = jnp.dot(nrm[r, :], mine[...], preferred_element_type=F32).astype(BF)

    stages(NC, (0, first), (1, gather.relay), (2, gather.far), (3, compute))
    weights.wait_theirs()

    def rest(t):
        r = flat_rows(t)[0]
        qkv[r, 384:768] = jnp.dot(nrm[r, :], theirs[...], preferred_element_type=F32).astype(BF)

    each(NC, rest)
    each(NC, gather.drain)

    @pl.when(p.c != p.zl)
    def _():
        each(NC, lambda t: swap(t).wait_send())

    weights.drain()


def lanes(rows):
    return lax.broadcasted_iota(jnp.int32, (rows, 128), 1)


def widen(qkv, vx):
    for pair in range(2):
        vx[pair, :, 0:128] = qkv[:, pair * 384 + 256 : pair * 384 + 384]
        vx[pair, :, 128:256] = jnp.ones((T, 128), BF)


def head_pair(q, k, v, mask):
    lane = lanes(q.shape[0])
    outs = []
    for a in range(2):
        qa = jnp.where((lane < 64) == (a == 0), q, jnp.zeros_like(q))
        s = lax.dot_general(qa, k, (((1,), (1,)), ((), ())), preferred_element_type=F32)
        if mask is not None:
            s = jnp.where(mask, s, -1e30)
        e = jnp.exp(s - jnp.max(s, axis=-1, keepdims=True)).astype(BF)
        o = jnp.dot(e, v, preferred_element_type=F32)
        outs.append(o[:, 0:128] / o[:, 128:256])
    return jnp.where(lane < 64, outs[0], outs[1]).astype(BF)


def attend_out(spatial, ch, gate_row, qkv, own, mod, w, extra, out, rider, *scratch):
    act, w2, part, fs, fr, ns, nr, rs_s, rs_r, vx, ws, wr, wl, es, er = scratch
    n = T // ch
    p = Place()
    greet([p.L, p.R, p.D, p.U, p.N])
    weights = Out(p, w, w2, 128, ws, wr, wl)
    reduce = Reduce(p, ch, act, 256, w2, part, fs, fr, ns, nr, rs_s, rs_r)
    for copy in weights.sends():
        copy.start()
    for copy in weights.locals():
        copy.start()
    if spatial:
        half = pl.ds(pl.multiple_of(p.c * 512, 512), 512)
        riders = [
            rc(
                extra.at[d * 1024 : d * 1024 + 1024, half], rider.at[d * 1024 : d * 1024 + 1024, :],
                es.at[d], er.at[d], (p.U, p.N)[d],
            )
            for d in range(2)
        ]
    else:
        riders = list(Out(p, extra, None, 512, es, er, None, rider).sends())
    for copy in riders:
        copy.start()
    widen(qkv, vx)
    if spatial:
        mask = None
    else:
        i = lax.broadcasted_iota(jnp.int32, (ch, ch), 0)
        j = lax.broadcasted_iota(jnp.int32, (ch, ch), 1)
        mask = lax.rem(i, 16) == lax.rem(j, 16)

    def heads(t):
        r = reduce.r(t)
        keys = slice(None) if spatial else r
        for pair in range(2):
            base = pair * 384
            q = qkv[r, base : base + 128] * jnp.array(0.125, BF)
            act[r, pair * 128 : pair * 128 + 128] = head_pair(
                q, qkv[keys, base + 128 : base + 256], vx[pair, keys, :], mask
            )
        reduce.share(t)

    def project(t):
        @pl.when(t == 0)
        def _():
            weights.wait_recv()
            for copy in weights.locals():
                copy.wait()

        reduce.project(t)

    gate = mod[gate_row : gate_row + 1, blk(p.x, p.c)]

    def finish(t):
        r = reduce.r(t)
        out[r, :] = (own[r, :].astype(F32) + gate * reduce.total(t)).astype(BF)

    stages(n, (0, heads), (1, project), (2, reduce.near), (3, finish))
    each(n, reduce.drain)
    weights.drain()
    for copy in riders:
        copy.wait()


def patch_rows(t):
    return (lax.div(t, 2), pl.ds(lax.rem(t, 2) * 8, 8), slice(None))


def temporal_in(stream, mod, w, qkv, own, full, nrm, mine, theirs, gs, gr, ws, wr, wl, ls, ss, sr):
    p = Place()
    peers = [p.row_dev(lax.rem(p.row + k, 16)) for k in range(1, 16)]
    greet([p.L, p.R, p.D] + peers)
    gather = Gather(p, full, patch_rows, gs, gr)
    weights = QKV(p, w, mine, theirs, ws, wr, wl)
    here = blk(p.x, p.c)

    def send(k):
        row = lax.rem(p.row + k, 16)
        return rc(
            stream.at[pl.ds(row * 4, 4), :, :], full.at[:, p.row, :, here],
            ss.at[k], sr.at[p.row], p.row_dev(row),
        )

    keep = pltpu.make_async_copy(stream.at[pl.ds(p.row * 4, 4), :, :], full.at[:, p.row, :, here], ls.at[0])
    each(15, lambda k: send(k + 1).start())
    keep.start()
    weights.start()

    def arrived(k):
        frame = lax.rem(p.row + k, 16)
        rc(
            stream.at[pl.ds(frame * 4, 4), :, :], full.at[:, frame, :, here],
            ss.at[k], sr.at[frame], p.row_dev(frame),
        ).wait_recv()

    keep.wait()
    each(15, lambda k: arrived(k + 1))

    def compute(t):
        gather.arrive(t)
        r = flat_rows(t)[0]
        index = patch_rows(t)
        nrm[r, :] = normed(full[(*index, slice(None))].reshape(CH, D), mod, 3)
        own[r, :] = full[(*index, here)].reshape(CH, B)

        @pl.when(t == 0)
        def _():
            weights.wait_mine()

        qkv[r, 0:384] = jnp.dot(nrm[r, :], mine[...], preferred_element_type=F32).astype(BF)

    stages(NC, (0, gather.own), (1, gather.relay), (2, gather.far), (3, compute))
    weights.wait_theirs()

    def rest(t):
        r = flat_rows(t)[0]
        qkv[r, 384:768] = jnp.dot(nrm[r, :], theirs[...], preferred_element_type=F32).astype(BF)

    each(NC, rest)
    each(NC, gather.drain)
    each(15, lambda k: send(k + 1).wait_send())
    weights.drain()


def mlp(stream, mod, hw, hw_p, ow, ow_p, out, full, w1, res, *scratch):
    act, w2, part, fs, fr, ns, nr, rs_s, rs_r, gs, gr, wl, ls, ss, sr = scratch
    p = Place()
    greet([p.L, p.R, p.D, p.S])
    gather = Gather(p, full, flat_rows, gs, gr)
    reduce = Reduce(p, CH, act, 1024, w2, part, fs, fr, ns, nr, rs_s, rs_r)
    here = blk(p.x, p.c)
    weights = Out(p, ow, w2, 512, None, None, wl)
    half = pl.ds(pl.multiple_of(p.c * 512, 512), 512)
    first = [
        pltpu.make_async_copy(hw.at[:, half], w1.at[:, 0:512], wl.at[8]),
        pltpu.make_async_copy(hw_p, w1.at[:, 512:1024], wl.at[9]),
    ]
    second = list(weights.locals()) + [
        pltpu.make_async_copy(ow_p.at[0:512, :], w2.at[512:1024, :], wl.at[10]),
        pltpu.make_async_copy(ow_p.at[512:1024, :], w2.at[1536:2048, :], wl.at[11]),
    ]

    def keep(t):
        r = flat_rows(t)[0]
        return pltpu.make_async_copy(stream.at[r, :], full.at[r, here], ls.at[t])

    each(NC, lambda t: keep(t).start())
    for copy in first + second:
        copy.start()

    def enter(t):
        keep(t).wait()
        gather.own(t)

    def hidden(t):
        @pl.when(t == 0)
        def _():
            for copy in first:
                copy.wait()

        gather.arrive(t)
        r = flat_rows(t)[0]
        h = jnp.dot(normed(full[r, :], mod, 6), w1[...], preferred_element_type=F32)
        h = 0.5 * h * (1.0 + jnp.tanh(0.7978845608028654 * (h + 0.044715 * (h * h * h))))
        act[r, 0:1024] = h.astype(BF)
        reduce.share(t)

    def project(t):
        @pl.when(t == 0)
        def _():
            for copy in second:
                copy.wait()

        reduce.project(t)

    gate = mod[8:9, here]

    def ends(t):
        src = res.at[pl.ds(t * 8, 8), :, :]
        dst = out.at[pl.ds(lax.rem(t, 2) * 8, 8), pl.ds(pl.multiple_of(lax.div(t, 2) * 16, 16), 16), :]
        return src, dst

    def put(t):
        return pltpu.make_async_copy(*ends(t), ls.at[t])

    def back(t):
        return rc(*ends(t), ss.at[t], sr.at[t], p.S)

    def finish(t):
        r = flat_rows(t)[0]
        value = full[r, here].astype(F32) + gate * reduce.total(t)
        res[pl.ds(t * 8, 8), :, :] = value.astype(BF).reshape(8, 16, B)

        @pl.when(p.c == p.zl)
        def _():
            put(t).start()

        @pl.when(p.c != p.zl)
        def _():
            back(t).start()

    stages(
        NC, (0, enter), (1, gather.relay), (2, gather.far), (3, hidden), (4, project), (5, reduce.near), (6, finish)
    )
    each(NC, gather.drain)
    each(NC, reduce.drain)

    @pl.when(p.c == p.zl)
    def _():
        each(NC, lambda t: put(t).wait())

    @pl.when(p.c != p.zl)
    def _():
        each(NC, lambda t: back(t).wait())


def call(kernel, name, ident, ins, outs, scratch, limit, cost):
    return pl.pallas_call(
        kernel,
        name=name,
        out_shape=[jax.ShapeDtypeStruct(shape, BF) for shape, _ in outs],
        in_specs=ins,
        out_specs=[spec for _, spec in outs],
        scratch_shapes=scratch,
        compiler_params=pltpu.CompilerParams(
            collective_id=ident, has_side_effects=True, vmem_limit_bytes=limit << 20
        ),
        cost_estimate=pl.CostEstimate(flops=cost, bytes_accessed=1 << 24, transcendentals=0),
    )


def gather_scratch(full):
    return [
        VM(full, BF), VM((T, D), BF), VM((D, 384), BF), VM((D, 384), BF),
        DMA((9, NC)), DMA((9, NC)), DMA((6,)), DMA((6,)), DMA((3,)), DMA((NC,)),
    ]


def per_device(latent, mod, sqkv, so, tqkv, to, hw, ow):
    qkv_shape, block = (T, 768), (T, B)
    qkv, own = call(
        spatial_in, "spatial_in", 0, [ANY, INV, ANY], [(qkv_shape, INV), (block, INV)],
        gather_scratch((T, D)) + [DMA((NC,)), DMA((NC,))], 40, 10**10,
    )(latent, mod, sqkv)

    def attend(spatial, ch, row, ident, qkv, own, w, extra):
        n = T // ch
        rider = ((D, 512), ANY) if spatial else ((1024, 1024), ANY)
        return call(
            functools.partial(attend_out, spatial, ch, row), "spatial_out" if spatial else "temporal_out", ident,
            [INV, INV, INV, ANY, ANY], [(block, INV), rider],
            reduce_scratch(n, 512)
            + [VM((2, T, B), BF), DMA((8,)), DMA((8,)), DMA((8,)), DMA((8,)), DMA((8,))],
            40, 10**10,
        )(qkv, own, mod, w, extra)

    one, hw_p = attend(True, 128, 2, 1, qkv, own, so, hw)
    qkv, own = call(
        temporal_in, "temporal_in", 2, [INV, INV, ANY], [(qkv_shape, INV), (block, INV)],
        gather_scratch((4, 16, 16, D)) + [DMA((16,)), DMA((16,))], 40, 10**10,
    )(one.reshape(64, 16, B), mod, tqkv)
    two, ow_p = attend(False, 256, 5, 3, qkv, own, to, ow)
    (out,) = call(
        mlp, "mlp", 4, [INV, INV, ANY, ANY, ANY, ANY], [((16, 64, B), ANY)],
        [VM((T, D), BF), VM((D, 1024), BF), VM((64, 16, B), BF)]
        + reduce_scratch(NC, 2048)
        + [DMA((9, NC)), DMA((9, NC)), DMA((12,)), DMA((NC,)), DMA((NC,)), DMA((NC,))],
        48, 2 * 10**10,
    )(two, mod, hw, hw_p, ow, ow_p)
    return out


def solution(mesh):
    in_specs = (
        P("seq", None, "head"), P(), P(None, None, "head"), P("head", None),
        P(None, None, "head"), P("head", None), P(None, "head"), P("head", None),
    )
    return jax.shard_map(
        per_device, mesh=mesh, in_specs=in_specs, out_specs=P(None, "seq", "head"), check_vma=False
    )
```

```python
import functools

import jax
import jax.numpy as jnp
from jax import lax
from jax.experimental import pallas as pl
from jax.experimental.pallas import tpu as pltpu
from jax.sharding import PartitionSpec as P

MESH = pl.DeviceIdType.MESH
BF = jnp.bfloat16
F32 = jnp.float32
T = 1024
D = 2048
B = 256
VM = pltpu.VMEM
ANY = pl.BlockSpec(memory_space=pltpu.MemorySpace.HBM)
INV = pl.BlockSpec(memory_space=pltpu.VMEM)


def rc(src, dst, ss, rs, dev):
    return pltpu.make_async_remote_copy(
        src_ref=src, dst_ref=dst, send_sem=ss, recv_sem=rs, device_id=dev, device_id_type=MESH
    )


class Place:
    def __init__(self):
        s, h = lax.axis_index("seq"), lax.axis_index("head")
        self.c, self.y, self.zh = lax.rem(s, 2), lax.rem(lax.div(s, 2), 4), lax.div(s, 8)
        self.x, self.zl = lax.div(h, 2), lax.rem(h, 2)
        self.z = self.zh * 2 + self.zl
        self.o = 1 - self.c
        self.row = (self.zh * 4 + self.y) * 2 + self.zl
        self.xr, self.xl, self.xf = [lax.rem(self.x + k, 4) for k in (1, 3, 2)]
        self.R = self.dev(self.xr, self.z, self.c)
        self.L = self.dev(self.xl, self.z, self.c)
        self.D = self.dev(self.x, self.z, self.o)
        self.U = self.dev(self.x, lax.rem(self.z + 1, 4), self.c)
        self.N = self.dev(self.x, lax.rem(self.z + 3, 4), self.c)
        self.S = ((self.zh * 4 + self.y) * 2 + self.o, self.x * 2 + 1 - self.zl)

    def dev(self, x, z, c):
        return ((lax.div(z, 2) * 4 + self.y) * 2 + c, x * 2 + lax.rem(z, 2))

    def row_dev(self, row):
        return (lax.div(row, 2) * 2 + self.c, self.x * 2 + lax.rem(row, 2))


def greet(devices):
    barrier = pltpu.get_barrier_semaphore()
    for device in devices:
        pl.semaphore_signal(barrier, inc=1, device_id=device, device_id_type=MESH)
    pl.semaphore_wait(barrier, len(devices))


def blk(x, c, width=B, off=0):
    return pl.ds(pl.multiple_of((x * 2 + c) * B + off, 128), width)


class Gather:
    KINDS = 9

    def __init__(self, p, full, rows, ss, rs):
        self.p, self.full, self.rows, self.ss, self.rs = p, full, rows, ss, rs
        x, c, o = p.x, p.c, p.o
        H = 128
        self.sent = [
            (blk(x, c), p.R), (blk(x, c), p.L), (blk(x, c), p.D),
            (blk(p.xl, c, H), p.R), (blk(p.xr, c, H, H), p.L),
            (blk(p.xl, c), p.D), (blk(p.xr, c), p.D),
            (blk(p.xf, c, H), p.D), (blk(p.xf, c, H, H), p.D),
        ]
        self.landed = [
            blk(p.xl, c), blk(p.xr, c), blk(x, o),
            blk(p.xf, c, H), blk(p.xf, c, H, H),
            blk(p.xl, o), blk(p.xr, o),
            blk(p.xf, o, H), blk(p.xf, o, H, H),
        ]

    def out(self, k, t):
        cols, dev = self.sent[k]
        ref = self.full.at[(*self.rows(t), cols)]
        return rc(ref, ref, self.ss.at[k, t], self.rs.at[k, t], dev)

    def got(self, k, t):
        ref = self.full.at[(*self.rows(t), self.landed[k])]
        rc(ref, ref, self.ss.at[k, t], self.rs.at[k, t], self.sent[k][1]).wait_recv()

    def own(self, t):
        for k in (0, 1, 2):
            self.out(k, t).start()

    def relay(self, t):
        self.got(0, t)
        self.out(3, t).start()
        self.out(5, t).start()
        self.got(1, t)
        self.out(4, t).start()
        self.out(6, t).start()

    def far(self, t):
        self.got(3, t)
        self.out(7, t).start()
        self.got(4, t)
        self.out(8, t).start()

    def arrive(self, t):
        for k in (2, 5, 6, 7, 8):
            self.got(k, t)

    def drain(self, t):
        for k in range(9):
            self.out(k, t).wait_send()


class Reduce:
    def __init__(self, p, ch, act, half, w, part, fs, fr, ns, nr, ss, rs):
        self.p, self.ch, self.act, self.half, self.w, self.part = p, ch, act, half, w, part
        self.fs, self.fr, self.ns, self.nr, self.ss, self.rs = fs, fr, ns, nr, ss, rs

    def r(self, t):
        return pl.ds(pl.multiple_of(t * self.ch, self.ch), self.ch)

    def copy(self, k, t):
        p, r = self.p, self.r(t)
        if k == 0:
            src, dst, dev = self.act.at[r, 0 : self.half], self.act.at[r, self.half : 2 * self.half], p.D
        elif k in (1, 2):
            src, dst, dev = self.fs.at[k - 1, r], self.fr.at[k - 1, r], (p.R, p.L)[k - 1]
        else:
            src, dst, dev = self.ns.at[k - 3, r], self.nr.at[k - 3, r], (p.R, p.L)[k - 3]
        return rc(src, dst, self.ss.at[k, t], self.rs.at[k, t], dev)

    def share(self, t):
        self.copy(0, t).start()

    def project(self, t):
        r = self.r(t)
        self.copy(0, t).wait_recv()
        out = jnp.dot(self.act[r, :], self.w[...], preferred_element_type=F32)
        self.fs[0, r] = out[:, 512:640].astype(BF)
        self.fs[1, r] = out[:, 640:768].astype(BF)
        self.copy(1, t).start()
        self.copy(2, t).start()
        self.part[r, 0:512] = out[:, 0:512]
        self.part[r, 512:768] = out[:, 768:1024]

    def near(self, t):
        r = self.r(t)
        self.copy(1, t).wait_recv()
        self.ns[0, r, 0:128] = (self.part[r, 256:384] + self.fr[0, r].astype(F32)).astype(BF)
        self.ns[0, r, 128:256] = self.part[r, 384:512].astype(BF)
        self.copy(3, t).start()
        self.copy(2, t).wait_recv()
        self.ns[1, r, 0:128] = self.part[r, 512:640].astype(BF)
        self.ns[1, r, 128:256] = (self.part[r, 640:768] + self.fr[1, r].astype(F32)).astype(BF)
        self.copy(4, t).start()

    def total(self, t):
        r = self.r(t)
        self.copy(3, t).wait_recv()
        self.copy(4, t).wait_recv()
        return self.part[r, 0:256] + self.nr[0, r].astype(F32) + self.nr[1, r].astype(F32)

    def drain(self, t):
        for k in range(5):
            self.copy(k, t).wait_send()


def reduce_scratch(nc, width):
    return [
        VM((T, width), BF), VM((width, 1024), BF), VM((T, 768), F32),
        VM((2, T, 128), BF), VM((2, T, 128), BF), VM((2, T, B), BF), VM((2, T, B), BF),
        pltpu.SemaphoreType.DMA((5, nc)), pltpu.SemaphoreType.DMA((5, nc)),
    ]


def normed(values, mod, row):
    v = values.astype(F32)
    v = v - jnp.mean(v, axis=-1, keepdims=True)
    v = v * lax.rsqrt(jnp.mean(v * v, axis=-1, keepdims=True) + 1e-06)
    return (v * (1.0 + mod[row + 1 : row + 2, :]) + mod[row : row + 1, :]).astype(BF)


def stages(n, *steps):
    last = max(lag for lag, _ in steps)

    def body(i, carry):
        for lag, function in steps:
            t = i - lag

            @pl.when((t >= 0) & (t < n))
            def _(t=t, function=function):
                function(t)

        return carry

    lax.fori_loop(0, n + last, body, 0)


def each(n, function):
    def body(i, carry):
        function(i)
        return carry

    lax.fori_loop(0, n, body, 0)


class QKV:
    def __init__(self, p, w, mine, theirs, ss, rs, ls):
        self.p, self.w, self.mine, self.theirs, self.ss, self.rs, self.ls = p, w, mine, theirs, ss, rs, ls

    def pieces(self):
        half = pl.ds(pl.multiple_of(self.p.c * 128, 128), 128)
        for j in range(3):
            yield j, self.ls.at[j], pltpu.make_async_copy(
                self.w.at[j, :, half], self.mine.at[:, j * 128 : j * 128 + 128], self.ls.at[j]
            )

    def sends(self):
        half = pl.ds(pl.multiple_of(self.p.c * 128, 128), 128)
        for j in range(3):
            for d, dev in enumerate((self.p.U, self.p.N)):
                yield rc(
                    self.w.at[j, d * 1024 : d * 1024 + 1024, half],
                    self.theirs.at[d * 1024 : d * 1024 + 1024, j * 128 : j * 128 + 128],
                    self.ss.at[j * 2 + d], self.rs.at[j * 2 + d], dev,
                )

    def start(self):
        for copy in self.sends():
            copy.start()
        for _, _, copy in self.pieces():
            copy.start()

    def wait_mine(self):
        for _, _, copy in self.pieces():
            copy.wait()

    def wait_theirs(self):
        for copy in self.sends():
            copy.wait_recv()

    def drain(self):
        for copy in self.sends():
            copy.wait_send()


class Out:
    def __init__(self, p, w, dst, rows, ss, rs, ls, stage=None):
        self.p, self.w, self.dst, self.rows, self.ss, self.rs, self.ls, self.stage = p, w, dst, rows, ss, rs, ls, stage

    def src(self, g, j):
        half = (self.p.c, self.p.o)[g]
        n = self.rows
        return self.w.at[pl.ds(pl.multiple_of(half * n, n), n), blk(lax.rem(self.p.x + j, 4), self.p.c)]

    def locals(self):
        n = self.rows
        for g in range(2):
            for j in range(4):
                yield pltpu.make_async_copy(
                    self.src(g, j), self.dst.at[2 * g * n : 2 * g * n + n, j * B : j * B + B], self.ls.at[g * 4 + j]
                )

    def sends(self):
        n = self.rows
        for g in range(2):
            for j in range(4):
                if self.stage is None:
                    dst = self.dst.at[2 * g * n + n : 2 * g * n + 2 * n, j * B : j * B + B]
                else:
                    dst = self.stage.at[g * n : g * n + n, j * B : j * B + B]
                yield rc(
                    self.src(g, j), dst,
                    self.ss.at[g * 4 + j], self.rs.at[g * 4 + j], (self.p.U, self.p.N)[g],
                )

    def wait_recv(self):
        for copy in self.sends():
            copy.wait_recv()

    def drain(self):
        for copy in self.sends():
            copy.wait_send()


DMA = pltpu.SemaphoreType.DMA
NC, CH = 8, 128


def flat_rows(t):
    return (pl.ds(pl.multiple_of(t * CH, CH), CH),)


def spatial_in(latent, mod, w, qkv, own, full, nrm, mine, theirs, gs, gr, ws, wr, wl, ls, ss, sr):
    p = Place()
    greet([p.L, p.R, p.D, p.U, p.N, p.S])
    gather = Gather(p, full, flat_rows, gs, gr)
    weights = QKV(p, w, mine, theirs, ws, wr, wl)
    here = blk(p.x, p.c)

    def keep(t):
        r = flat_rows(t)[0]
        return pltpu.make_async_copy(latent.at[0, r, :], full.at[r, here], ls.at[t])

    def swap(t):
        r = flat_rows(t)[0]
        return rc(latent.at[0, r, :], full.at[r, blk(p.x, p.o)], ss.at[t], sr.at[t], p.S)

    def landed(t):
        r = flat_rows(t)[0]
        return rc(latent.at[0, r, :], full.at[r, here], ss.at[t], sr.at[t], p.S)

    @pl.when(p.c == p.zl)
    def _():
        each(NC, lambda t: keep(t).start())

    @pl.when(p.c != p.zl)
    def _():
        each(NC, lambda t: swap(t).start())

    weights.start()

    def first(t):
        @pl.when(p.c == p.zl)
        def _():
            keep(t).wait()

        @pl.when(p.c != p.zl)
        def _():
            landed(t).wait_recv()

        gather.own(t)

    def compute(t):
        gather.arrive(t)
        r = flat_rows(t)[0]
        nrm[r, :] = normed(full[r, :], mod, 0)
        own[r, :] = full[r, here]

        @pl.when(t == 0)
        def _():
            weights.wait_mine()

        qkv[r, 0:384] = jnp.dot(nrm[r, :], mine[...], preferred_element_type=F32).astype(BF)

    stages(NC, (0, first), (2, gather.relay), (4, gather.far), (6, compute))
    weights.wait_theirs()

    def rest(t):
        r = flat_rows(t)[0]
        qkv[r, 384:768] = jnp.dot(nrm[r, :], theirs[...], preferred_element_type=F32).astype(BF)

    each(NC, rest)
    each(NC, gather.drain)

    @pl.when(p.c != p.zl)
    def _():
        each(NC, lambda t: swap(t).wait_send())

    weights.drain()


def lanes(rows):
    return lax.broadcasted_iota(jnp.int32, (rows, 128), 1)


def widen(qkv, vx):
    for pair in range(2):
        vx[pair, :, 0:128] = qkv[:, pair * 384 + 256 : pair * 384 + 384]
        vx[pair, :, 128:256] = jnp.ones((T, 128), BF)


def head_pair(q, k, v, mask):
    lane = lanes(q.shape[0])
    outs = []
    for a in range(2):
        qa = jnp.where((lane < 64) == (a == 0), q, jnp.zeros_like(q))
        s = lax.dot_general(qa, k, (((1,), (1,)), ((), ())), preferred_element_type=F32)
        if mask is not None:
            s = jnp.where(mask, s, -1e30)
        e = jnp.exp(s - jnp.max(s, axis=-1, keepdims=True)).astype(BF)
        o = jnp.dot(e, v, preferred_element_type=F32)
        outs.append(o[:, 0:128] / o[:, 128:256])
    return jnp.where(lane < 64, outs[0], outs[1]).astype(BF)


def attend_out(spatial, ch, gate_row, qkv, own, mod, w, extra, out, rider, *scratch):
    act, w2, part, fs, fr, ns, nr, rs_s, rs_r, vx, ws, wr, wl, es, er = scratch
    n = T // ch
    p = Place()
    greet([p.L, p.R, p.D, p.U, p.N])
    weights = Out(p, w, w2, 128, ws, wr, wl)
    reduce = Reduce(p, ch, act, 256, w2, part, fs, fr, ns, nr, rs_s, rs_r)
    for copy in weights.sends():
        copy.start()
    for copy in weights.locals():
        copy.start()
    if spatial:
        half = pl.ds(pl.multiple_of(p.c * 512, 512), 512)
        riders = [
            rc(
                extra.at[d * 1024 : d * 1024 + 1024, half], rider.at[d * 1024 : d * 1024 + 1024, :],
                es.at[d], er.at[d], (p.U, p.N)[d],
            )
            for d in range(2)
        ]
    else:
        riders = list(Out(p, extra, None, 512, es, er, None, rider).sends())
    for copy in riders:
        copy.start()
    widen(qkv, vx)
    if spatial:
        mask = None
    else:
        i = lax.broadcasted_iota(jnp.int32, (ch, ch), 0)
        j = lax.broadcasted_iota(jnp.int32, (ch, ch), 1)
        mask = lax.rem(i, 16) == lax.rem(j, 16)

    def heads(t):
        r = reduce.r(t)
        keys = slice(None) if spatial else r
        for pair in range(2):
            base = pair * 384
            q = qkv[r, base : base + 128] * jnp.array(0.125, BF)
            act[r, pair * 128 : pair * 128 + 128] = head_pair(
                q, qkv[keys, base + 128 : base + 256], vx[pair, keys, :], mask
            )
        reduce.share(t)

    def project(t):
        @pl.when(t == 0)
        def _():
            weights.wait_recv()
            for copy in weights.locals():
                copy.wait()

        reduce.project(t)

    gate = mod[gate_row : gate_row + 1, blk(p.x, p.c)]

    def finish(t):
        r = reduce.r(t)
        out[r, :] = (own[r, :].astype(F32) + gate * reduce.total(t)).astype(BF)

    stages(n, (0, heads), *((2, project), (4, reduce.near), (6, finish)) if spatial else ((1, project), (2, reduce.near), (3, finish)))
    each(n, reduce.drain)
    weights.drain()
    for copy in riders:
        copy.wait()


def patch_rows(t):
    return (lax.div(t, 2), pl.ds(lax.rem(t, 2) * 8, 8), slice(None))


def temporal_in(stream, mod, w, qkv, own, full, nrm, mine, theirs, gs, gr, ws, wr, wl, ls, ss, sr):
    p = Place()
    peers = [p.row_dev(lax.rem(p.row + k, 16)) for k in range(1, 16)]
    greet([p.L, p.R, p.D] + peers)
    gather = Gather(p, full, patch_rows, gs, gr)
    weights = QKV(p, w, mine, theirs, ws, wr, wl)
    here = blk(p.x, p.c)

    def send(k):
        row = lax.rem(p.row + k, 16)
        return rc(
            stream.at[pl.ds(row * 4, 4), :, :], full.at[:, p.row, :, here],
            ss.at[k], sr.at[p.row], p.row_dev(row),
        )

    keep = pltpu.make_async_copy(stream.at[pl.ds(p.row * 4, 4), :, :], full.at[:, p.row, :, here], ls.at[0])
    each(15, lambda k: send(k + 1).start())
    keep.start()
    weights.start()

    def arrived(k):
        frame = lax.rem(p.row + k, 16)
        rc(
            stream.at[pl.ds(frame * 4, 4), :, :], full.at[:, frame, :, here],
            ss.at[k], sr.at[frame], p.row_dev(frame),
        ).wait_recv()

    keep.wait()
    each(15, lambda k: arrived(k + 1))

    def compute(t):
        gather.arrive(t)
        r = flat_rows(t)[0]
        index = patch_rows(t)
        nrm[r, :] = normed(full[(*index, slice(None))].reshape(CH, D), mod, 3)
        own[r, :] = full[(*index, here)].reshape(CH, B)

        @pl.when(t == 0)
        def _():
            weights.wait_mine()

        qkv[r, 0:384] = jnp.dot(nrm[r, :], mine[...], preferred_element_type=F32).astype(BF)

    stages(NC, (0, gather.own), (3, gather.relay), (5, gather.far), (6, compute))
    weights.wait_theirs()

    def rest(t):
        r = flat_rows(t)[0]
        qkv[r, 384:768] = jnp.dot(nrm[r, :], theirs[...], preferred_element_type=F32).astype(BF)

    each(NC, rest)
    each(NC, gather.drain)
    each(15, lambda k: send(k + 1).wait_send())
    weights.drain()


def mlp(stream, mod, hw, hw_p, ow, ow_p, out, full, w1, res, *scratch):
    act, w2, part, fs, fr, ns, nr, rs_s, rs_r, gs, gr, wl, ls, ss, sr = scratch
    p = Place()
    greet([p.L, p.R, p.D, p.S])
    gather = Gather(p, full, flat_rows, gs, gr)
    reduce = Reduce(p, CH, act, 1024, w2, part, fs, fr, ns, nr, rs_s, rs_r)
    here = blk(p.x, p.c)
    weights = Out(p, ow, w2, 512, None, None, wl)
    half = pl.ds(pl.multiple_of(p.c * 512, 512), 512)
    first = [
        pltpu.make_async_copy(hw.at[:, half], w1.at[:, 0:512], wl.at[8]),
        pltpu.make_async_copy(hw_p, w1.at[:, 512:1024], wl.at[9]),
    ]
    second = list(weights.locals()) + [
        pltpu.make_async_copy(ow_p.at[0:512, :], w2.at[512:1024, :], wl.at[10]),
        pltpu.make_async_copy(ow_p.at[512:1024, :], w2.at[1536:2048, :], wl.at[11]),
    ]

    def keep(t):
        r = flat_rows(t)[0]
        return pltpu.make_async_copy(stream.at[r, :], full.at[r, here], ls.at[t])

    each(NC, lambda t: keep(t).start())
    for copy in first + second:
        copy.start()

    def enter(t):
        keep(t).wait()
        gather.own(t)

    def hidden(t):
        @pl.when(t == 0)
        def _():
            for copy in first:
                copy.wait()

        gather.arrive(t)
        r = flat_rows(t)[0]
        h = jnp.dot(normed(full[r, :], mod, 6), w1[...], preferred_element_type=F32)
        h = 0.5 * h * (1.0 + jnp.tanh(0.7978845608028654 * (h + 0.044715 * (h * h * h))))
        act[r, 0:1024] = h.astype(BF)
        reduce.share(t)

    def project(t):
        @pl.when(t == 0)
        def _():
            for copy in second:
                copy.wait()

        reduce.project(t)

    gate = mod[8:9, here]

    def ends(t):
        src = res.at[pl.ds(t * 8, 8), :, :]
        dst = out.at[pl.ds(lax.rem(t, 2) * 8, 8), pl.ds(pl.multiple_of(lax.div(t, 2) * 16, 16), 16), :]
        return src, dst

    def put(t):
        return pltpu.make_async_copy(*ends(t), ls.at[t])

    def back(t):
        return rc(*ends(t), ss.at[t], sr.at[t], p.S)

    def finish(t):
        r = flat_rows(t)[0]
        value = full[r, here].astype(F32) + gate * reduce.total(t)
        res[pl.ds(t * 8, 8), :, :] = value.astype(BF).reshape(8, 16, B)

        @pl.when(p.c == p.zl)
        def _():
            put(t).start()

        @pl.when(p.c != p.zl)
        def _():
            back(t).start()

    stages(
        NC, (0, enter), (3, gather.relay), (5, gather.far), (6, hidden), (7, project), (9, reduce.near), (11, finish)
    )
    each(NC, gather.drain)
    each(NC, reduce.drain)

    @pl.when(p.c == p.zl)
    def _():
        each(NC, lambda t: put(t).wait())

    @pl.when(p.c != p.zl)
    def _():
        each(NC, lambda t: back(t).wait())


def call(kernel, name, ident, ins, outs, scratch, limit, cost):
    return pl.pallas_call(
        kernel,
        name=name,
        out_shape=[jax.ShapeDtypeStruct(shape, BF) for shape, _ in outs],
        in_specs=ins,
        out_specs=[spec for _, spec in outs],
        scratch_shapes=scratch,
        compiler_params=pltpu.CompilerParams(
            collective_id=ident, has_side_effects=True, vmem_limit_bytes=limit << 20
        ),
        cost_estimate=pl.CostEstimate(flops=cost, bytes_accessed=1 << 24, transcendentals=0),
    )


def gather_scratch(full):
    return [
        VM(full, BF), VM((T, D), BF), VM((D, 384), BF), VM((D, 384), BF),
        DMA((9, NC)), DMA((9, NC)), DMA((6,)), DMA((6,)), DMA((3,)), DMA((NC,)),
    ]


def per_device(latent, mod, sqkv, so, tqkv, to, hw, ow):
    qkv_shape, block = (T, 768), (T, B)
    qkv, own = call(
        spatial_in, "spatial_in", 0, [ANY, INV, ANY], [(qkv_shape, INV), (block, INV)],
        gather_scratch((T, D)) + [DMA((NC,)), DMA((NC,))], 40, 10**10,
    )(latent, mod, sqkv)

    def attend(spatial, ch, row, ident, qkv, own, w, extra):
        n = T // ch
        rider = ((D, 512), ANY) if spatial else ((1024, 1024), ANY)
        return call(
            functools.partial(attend_out, spatial, ch, row), "spatial_out" if spatial else "temporal_out", ident,
            [INV, INV, INV, ANY, ANY], [(block, INV), rider],
            reduce_scratch(n, 512)
            + [VM((2, T, B), BF), DMA((8,)), DMA((8,)), DMA((8,)), DMA((8,)), DMA((8,))],
            40, 10**10,
        )(qkv, own, mod, w, extra)

    one, hw_p = attend(True, 128, 2, 1, qkv, own, so, hw)
    qkv, own = call(
        temporal_in, "temporal_in", 2, [INV, INV, ANY], [(qkv_shape, INV), (block, INV)],
        gather_scratch((4, 16, 16, D)) + [DMA((16,)), DMA((16,))], 40, 10**10,
    )(one.reshape(64, 16, B), mod, tqkv)
    two, ow_p = attend(False, 256, 5, 3, qkv, own, to, ow)
    (out,) = call(
        mlp, "mlp", 4, [INV, INV, ANY, ANY, ANY, ANY], [((16, 64, B), ANY)],
        [VM((T, D), BF), VM((D, 1024), BF), VM((64, 16, B), BF)]
        + reduce_scratch(NC, 2048)
        + [DMA((9, NC)), DMA((9, NC)), DMA((12,)), DMA((NC,)), DMA((NC,)), DMA((NC,))],
        48, 2 * 10**10,
    )(two, mod, hw, hw_p, ow, ow_p)
    return out


def solution(mesh):
    in_specs = (
        P("seq", None, "head"), P(), P(None, None, "head"), P("head", None),
        P(None, None, "head"), P("head", None), P(None, "head"), P("head", None),
    )
    return jax.shard_map(
        per_device, mesh=mesh, in_specs=in_specs, out_specs=P(None, "seq", "head"), check_vma=False
    )
```

```python
import functools

import jax
import jax.numpy as jnp
from jax import lax
from jax.experimental import pallas as pl
from jax.experimental.pallas import tpu as pltpu
from jax.sharding import PartitionSpec as P

MESH = pl.DeviceIdType.MESH
BF = jnp.bfloat16
F32 = jnp.float32
T = 1024
D = 2048
B = 256
VM = pltpu.VMEM
ANY = pl.BlockSpec(memory_space=pltpu.MemorySpace.HBM)
INV = pl.BlockSpec(memory_space=pltpu.VMEM)


def rc(src, dst, ss, rs, dev):
    return pltpu.make_async_remote_copy(
        src_ref=src, dst_ref=dst, send_sem=ss, recv_sem=rs, device_id=dev, device_id_type=MESH
    )


class Place:
    def __init__(self):
        s, h = lax.axis_index("seq"), lax.axis_index("head")
        self.c, self.y, self.zh = lax.rem(s, 2), lax.rem(lax.div(s, 2), 4), lax.div(s, 8)
        self.x, self.zl = lax.div(h, 2), lax.rem(h, 2)
        self.z = self.zh * 2 + self.zl
        self.o = 1 - self.c
        self.row = (self.zh * 4 + self.y) * 2 + self.zl
        self.xr, self.xl, self.xf = [lax.rem(self.x + k, 4) for k in (1, 3, 2)]
        self.R = self.dev(self.xr, self.z, self.c)
        self.L = self.dev(self.xl, self.z, self.c)
        self.D = self.dev(self.x, self.z, self.o)
        self.U = self.dev(self.x, lax.rem(self.z + 1, 4), self.c)
        self.N = self.dev(self.x, lax.rem(self.z + 3, 4), self.c)
        self.S = ((self.zh * 4 + self.y) * 2 + self.o, self.x * 2 + 1 - self.zl)

    def dev(self, x, z, c):
        return ((lax.div(z, 2) * 4 + self.y) * 2 + c, x * 2 + lax.rem(z, 2))

    def row_dev(self, row):
        return (lax.div(row, 2) * 2 + self.c, self.x * 2 + lax.rem(row, 2))


def greet(devices):
    barrier = pltpu.get_barrier_semaphore()
    for device in devices:
        pl.semaphore_signal(barrier, inc=1, device_id=device, device_id_type=MESH)
    pl.semaphore_wait(barrier, len(devices))


def blk(x, c, width=B, off=0):
    return pl.ds(pl.multiple_of((x * 2 + c) * B + off, 128), width)


class Gather:
    KINDS = 9

    def __init__(self, p, full, rows, ss, rs):
        self.p, self.full, self.rows, self.ss, self.rs = p, full, rows, ss, rs
        x, c, o = p.x, p.c, p.o
        H = 128
        self.sent = [
            (blk(x, c), p.R), (blk(x, c), p.L), (blk(x, c), p.D),
            (blk(p.xl, c, H), p.R), (blk(p.xr, c, H, H), p.L),
            (blk(p.xl, c), p.D), (blk(p.xr, c), p.D),
            (blk(p.xf, c, H), p.D), (blk(p.xf, c, H, H), p.D),
        ]
        self.landed = [
            blk(p.xl, c), blk(p.xr, c), blk(x, o),
            blk(p.xf, c, H), blk(p.xf, c, H, H),
            blk(p.xl, o), blk(p.xr, o),
            blk(p.xf, o, H), blk(p.xf, o, H, H),
        ]

    def out(self, k, t):
        cols, dev = self.sent[k]
        ref = self.full.at[(*self.rows(t), cols)]
        return rc(ref, ref, self.ss.at[k, t], self.rs.at[k, t], dev)

    def got(self, k, t):
        ref = self.full.at[(*self.rows(t), self.landed[k])]
        rc(ref, ref, self.ss.at[k, t], self.rs.at[k, t], self.sent[k][1]).wait_recv()

    def own(self, t):
        for k in (0, 1, 2):
            self.out(k, t).start()

    def relay(self, t):
        self.got(0, t)
        self.out(3, t).start()
        self.out(5, t).start()
        self.got(1, t)
        self.out(4, t).start()
        self.out(6, t).start()

    def far(self, t):
        self.got(3, t)
        self.out(7, t).start()
        self.got(4, t)
        self.out(8, t).start()

    def arrive(self, t):
        for k in (2, 5, 6, 7, 8):
            self.got(k, t)

    def drain(self, t):
        for k in range(9):
            self.out(k, t).wait_send()


class Reduce:
    def __init__(self, p, ch, act, half, w, part, fs, fr, ns, nr, ss, rs):
        self.p, self.ch, self.act, self.half, self.w, self.part = p, ch, act, half, w, part
        self.fs, self.fr, self.ns, self.nr, self.ss, self.rs = fs, fr, ns, nr, ss, rs

    def r(self, t):
        return pl.ds(pl.multiple_of(t * self.ch, self.ch), self.ch)

    def copy(self, k, t):
        p, r = self.p, self.r(t)
        if k == 0:
            src, dst, dev = self.act.at[r, 0 : self.half], self.act.at[r, self.half : 2 * self.half], p.D
        elif k in (1, 2):
            src, dst, dev = self.fs.at[k - 1, r], self.fr.at[k - 1, r], (p.R, p.L)[k - 1]
        else:
            src, dst, dev = self.ns.at[k - 3, r], self.nr.at[k - 3, r], (p.R, p.L)[k - 3]
        return rc(src, dst, self.ss.at[k, t], self.rs.at[k, t], dev)

    def share(self, t):
        self.copy(0, t).start()

    def project(self, t):
        r = self.r(t)
        self.copy(0, t).wait_recv()
        out = jnp.dot(self.act[r, :], self.w[...], preferred_element_type=F32)
        self.fs[0, r] = out[:, 512:640].astype(BF)
        self.fs[1, r] = out[:, 640:768].astype(BF)
        self.copy(1, t).start()
        self.copy(2, t).start()
        self.part[r, 0:512] = out[:, 0:512]
        self.part[r, 512:768] = out[:, 768:1024]

    def near(self, t):
        r = self.r(t)
        self.copy(1, t).wait_recv()
        self.ns[0, r, 0:128] = (self.part[r, 256:384] + self.fr[0, r].astype(F32)).astype(BF)
        self.ns[0, r, 128:256] = self.part[r, 384:512].astype(BF)
        self.copy(3, t).start()
        self.copy(2, t).wait_recv()
        self.ns[1, r, 0:128] = self.part[r, 512:640].astype(BF)
        self.ns[1, r, 128:256] = (self.part[r, 640:768] + self.fr[1, r].astype(F32)).astype(BF)
        self.copy(4, t).start()

    def total(self, t):
        r = self.r(t)
        self.copy(3, t).wait_recv()
        self.copy(4, t).wait_recv()
        return self.part[r, 0:256] + self.nr[0, r].astype(F32) + self.nr[1, r].astype(F32)

    def drain(self, t):
        for k in range(5):
            self.copy(k, t).wait_send()


def normed(values, mod, row):
    v = values.astype(F32)
    v = v - jnp.mean(v, axis=-1, keepdims=True)
    v = v * lax.rsqrt(jnp.mean(v * v, axis=-1, keepdims=True) + 1e-06)
    return (v * (1.0 + mod[row + 1 : row + 2, :]) + mod[row : row + 1, :]).astype(BF)


def stages(n, *steps):
    last = max(lag for lag, _ in steps)

    def body(i, carry):
        for lag, function in steps:
            t = i - lag

            @pl.when((t >= 0) & (t < n))
            def _(t=t, function=function):
                function(t)

        return carry

    lax.fori_loop(0, n + last, body, 0)


def each(n, function):
    def body(i, carry):
        function(i)
        return carry

    lax.fori_loop(0, n, body, 0)


class QKV:
    def __init__(self, p, w, mine, theirs, ss, rs, ls):
        self.p, self.w, self.mine, self.theirs, self.ss, self.rs, self.ls = p, w, mine, theirs, ss, rs, ls
        self.half = pl.ds(pl.multiple_of(p.c * 128, 128), 128)

    def locals(self):
        return [
            pltpu.make_async_copy(self.w.at[j, :, self.half], self.mine.at[:, j * 128 : j * 128 + 128], self.ls.at[j])
            for j in range(3)
        ]

    def piece(self, i):
        for d, dev in enumerate((self.p.U, self.p.N)):
            rows = pl.ds(pl.multiple_of(d * 1024 + i * 128, 128), 128)
            for j in range(3):
                rc(
                    self.w.at[j, rows, self.half], self.theirs.at[rows, j * 128 : j * 128 + 128],
                    self.ss.at[d], self.rs.at[d], dev,
                ).start()

    def whole(self, d):
        ref = self.theirs.at[d * 1024 : d * 1024 + 1024, :]
        return rc(ref, ref, self.ss.at[d], self.rs.at[d], (self.p.U, self.p.N)[d])


class Out:
    def __init__(self, p, w, dst, rows, ss, rs, ls):
        self.p, self.w, self.dst, self.rows, self.ss, self.rs, self.ls = p, w, dst, rows, ss, rs, ls

    def src(self, g, j, first, count):
        start = (self.p.c, self.p.o)[g] * self.rows + first
        return self.w.at[pl.ds(pl.multiple_of(start, 128), count), blk(lax.rem(self.p.x + j, 4), self.p.c)]

    def locals(self):
        n = self.rows
        return [
            pltpu.make_async_copy(
                self.src(g, j, 0, n), self.dst.at[2 * g * n : 2 * g * n + n, j * B : j * B + B], self.ls.at[g * 4 + j]
            )
            for g in range(2)
            for j in range(4)
        ]

    def piece(self, i):
        n = self.rows
        per = n // 128
        j, first = lax.div(i, per), lax.rem(i, per) * 128
        for g, dev in enumerate((self.p.U, self.p.N)):
            rows = pl.ds(pl.multiple_of((2 * g + 1) * n + first, 128), 128)
            rc(
                self.src(g, j, first, 128), self.dst.at[rows, pl.ds(pl.multiple_of(j * B, B), B)],
                self.ss.at[g], self.rs.at[g], dev,
            ).start()

    def whole(self, g):
        n = self.rows
        ref = self.dst.at[(2 * g + 1) * n : (2 * g + 2) * n, :]
        return rc(ref, ref, self.ss.at[g], self.rs.at[g], (self.p.U, self.p.N)[g])


class Hidden:
    def __init__(self, p, w, dst, ss, rs, ls):
        self.p, self.w, self.dst, self.ss, self.rs, self.ls = p, w, dst, ss, rs, ls
        self.half = pl.ds(pl.multiple_of(p.c * 512, 512), 512)

    def locals(self):
        return [pltpu.make_async_copy(self.w.at[:, self.half], self.dst.at[:, 0:512], self.ls.at[0])]

    def piece(self, i):
        for d, dev in enumerate((self.p.U, self.p.N)):
            rows = pl.ds(pl.multiple_of(d * 1024 + i * 64, 64), 64)
            rc(
                self.w.at[rows, self.half], self.dst.at[rows, 512:1024], self.ss.at[d], self.rs.at[d], dev
            ).start()

    def whole(self, d):
        ref = self.dst.at[d * 1024 : d * 1024 + 1024, 512:1024]
        return rc(ref, ref, self.ss.at[d], self.rs.at[d], (self.p.U, self.p.N)[d])


def ready(weights):
    for d in range(2):
        weights.whole(d).wait_recv()
    for copy in weights.locals():
        copy.wait()


DMA = pltpu.SemaphoreType.DMA
NC, CH = 8, 128


def rows_of(t):
    return pl.ds(pl.multiple_of(t * CH, CH), CH)


def flat_rows(t):
    return (rows_of(t),)


def spatial_in(latent, mod, w, qkv, own, full, nrm, mine, theirs, gs, gr, ws, wr, wl, ls, ss, sr):
    p = Place()
    greet([p.L, p.R, p.D, p.U, p.N, p.S])
    gather = Gather(p, full, flat_rows, gs, gr)
    weights = QKV(p, w, mine, theirs, ws, wr, wl)
    here = blk(p.x, p.c)

    def keep(t):
        r = rows_of(t)
        return pltpu.make_async_copy(latent.at[r, :], full.at[r, here], ls.at[t])

    def swap(t):
        r = rows_of(t)
        return rc(latent.at[r, :], full.at[r, blk(p.x, p.o)], ss.at[t], sr.at[t], p.S)

    def landed(t):
        r = rows_of(t)
        return rc(latent.at[r, :], full.at[r, here], ss.at[t], sr.at[t], p.S)

    @pl.when(p.c == p.zl)
    def _():
        each(NC, lambda t: keep(t).start())

    @pl.when(p.c != p.zl)
    def _():
        each(NC, lambda t: swap(t).start())

    each(NC, weights.piece)
    for copy in weights.locals():
        copy.start()

    def first(t):
        @pl.when(p.c == p.zl)
        def _():
            keep(t).wait()

        @pl.when(p.c != p.zl)
        def _():
            landed(t).wait_recv()

        gather.own(t)

    def compute(t):
        gather.arrive(t)
        r = rows_of(t)
        nrm[r, :] = normed(full[r, :], mod, 0)
        own[r, :] = full[r, here]

        @pl.when(t == 0)
        def _():
            for copy in weights.locals():
                copy.wait()

        qkv[r, 0:384] = jnp.dot(nrm[r, :], mine[...], preferred_element_type=F32).astype(BF)

    stages(NC, (0, first), (2, gather.relay), (4, gather.far), (6, compute))
    for d in range(2):
        weights.whole(d).wait_recv()

    def rest(t):
        r = rows_of(t)
        qkv[r, 384:768] = jnp.dot(nrm[r, :], theirs[...], preferred_element_type=F32).astype(BF)

    each(NC, rest)
    each(NC, gather.drain)

    @pl.when(p.c != p.zl)
    def _():
        each(NC, lambda t: swap(t).wait_send())

    for d in range(2):
        weights.whole(d).wait_send()


def lanes(rows):
    return lax.broadcasted_iota(jnp.int32, (rows, 128), 1)


def head_pair(q, k, v, mask):
    lane = lanes(q.shape[0])
    outs = []
    for a in range(2):
        qa = jnp.where((lane < 64) == (a == 0), q, jnp.zeros_like(q))
        s = lax.dot_general(qa, k, (((1,), (1,)), ((), ())), preferred_element_type=F32)
        if mask is not None:
            s = jnp.where(mask, s, -1e30)
        e = jnp.exp(s - jnp.max(s, axis=-1, keepdims=True)).astype(BF)
        o = jnp.dot(e, v, preferred_element_type=F32)
        outs.append(o[:, 0:128] / o[:, 128:256])
    return jnp.where(lane < 64, outs[0], outs[1]).astype(BF)


PROJECT, NEAR, FINISH = 2, 4, 6
ENTER, RELAY, FAR, COMPUTE = 9, 11, 13, 15
PROJECT2, NEAR2, FINISH2 = 17, 19, 21
RELAY2, FAR2, COMPUTE2 = 23, 25, 27
PROJECT3, NEAR3, FINISH3 = 29, 31, 33


def tail(
    qkv, own, mod, so, tw, to, hw, ow, out,
    vx, ws, one, full1, mine, theirs, wt, full2, w1, w2, res, part,
    a1, fs1, fr1, ns1, nr1, a2, fs2, fr2, ns2, nr2, a3, fs3, fr3, ns3, nr3,
    s1, v1, s2, v2, s3, v3, g1, h1, g2, h2,
    ps, pr, qs, qr, us, ur, hs, hr, os, orr, pl_, ql, ul, hl, ol, xs, xr, ls, ss, sr,
):
    p = Place()
    greet([p.L, p.R, p.D, p.S] + [p.row_dev(lax.rem(p.row + k, 16)) for k in range(1, 16)])
    here = blk(p.x, p.c)
    wso = Out(p, so, ws, 128, ps, pr, pl_)
    wtq = QKV(p, tw, mine, theirs, qs, qr, ql)
    wto = Out(p, to, wt, 128, us, ur, ul)
    whi = Hidden(p, hw, w1, hs, hr, hl)
    wou = Out(p, ow, w2, 512, os, orr, ol)
    r1 = Reduce(p, CH, a1, 256, ws, part, fs1, fr1, ns1, nr1, s1, v1)
    r2 = Reduce(p, CH, a2, 256, wt, part, fs2, fr2, ns2, nr2, s2, v2)
    r3 = Reduce(p, CH, a3, 1024, w2, part, fs3, fr3, ns3, nr3, s3, v3)
    gat1 = Gather(p, full1, flat_rows, g1, h1)
    gat2 = Gather(p, full2, flat_rows, g2, h2)

    each(4, wso.piece)
    for weights in (wso, wtq, wto, whi, wou):
        for copy in weights.locals():
            copy.start()
    for pair in range(2):
        vx[pair, :, 0:128] = qkv[:, pair * 384 + 256 : pair * 384 + 384]
        vx[pair, :, 128:256] = jnp.ones((T, 128), BF)

    def heads(t):
        r = rows_of(t)
        for pair in range(2):
            base = pair * 384
            q = qkv[r, base : base + 128] * jnp.array(0.125, BF)
            a1[r, pair * 128 : pair * 128 + 128] = head_pair(q, qkv[:, base + 128 : base + 256], vx[pair], None)
        r1.share(t)

    def project1(t):
        @pl.when(t == 0)
        def _():
            ready(wso)

        r1.project(t)

    def eight(t, row):
        return pl.ds(pl.multiple_of(t * CH + row * 8, 8), 8)

    def cross(k, t):
        row = lax.rem(p.row + k, 16)
        return rc(one.at[eight(t, row), :], full1.at[eight(t, p.row), here], xs.at[k, t], xr.at[p.row, t], p.row_dev(row))

    def stay(t):
        return pltpu.make_async_copy(one.at[eight(t, p.row), :], full1.at[eight(t, p.row), here], xr.at[p.row, t])

    def finish1(t):
        r = rows_of(t)
        gate = mod[2:3, here]
        one[r, :] = (own[r, :].astype(F32) + gate * r1.total(t)).astype(BF)
        each(15, lambda k: cross(k + 1, t).start())
        stay(t).start()

    def enter1(t):
        def arrived(k):
            row = lax.rem(p.row + k, 16)
            rc(
                one.at[eight(t, row), :], full1.at[eight(t, row), here], xs.at[k, t], xr.at[row, t], p.row_dev(row)
            ).wait_recv()

        each(15, lambda k: arrived(k + 1))
        stay(t).wait()
        gat1.own(t)

    i = lax.broadcasted_iota(jnp.int32, (CH, CH), 0)
    j = lax.broadcasted_iota(jnp.int32, (CH, CH), 1)
    same = lax.rem(i, 8) == lax.rem(j, 8)

    def temporal(t):
        @pl.when(t == 0)
        def _():
            ready(wtq)

        gat1.arrive(t)
        r = rows_of(t)
        n = normed(full1[r, :], mod, 3)
        for pair, w in enumerate((mine, theirs)):
            y = jnp.dot(n, w[...], preferred_element_type=F32).astype(BF)
            v = jnp.concatenate([y[:, 256:384], jnp.ones((CH, 128), BF)], axis=1)
            a2[r, pair * 128 : pair * 128 + 128] = head_pair(
                y[:, 0:128] * jnp.array(0.125, BF), y[:, 128:256], v, same
            )
        r2.share(t)

    def project2(t):
        @pl.when(t == 0)
        def _():
            ready(wto)

        r2.project(t)

    def finish2(t):
        r = rows_of(t)
        gate = mod[5:6, here]
        full2[r, here] = (full1[r, here].astype(F32) + gate * r2.total(t)).astype(BF)
        gat2.own(t)

    def hidden(t):
        @pl.when(t == 0)
        def _():
            ready(whi)

        gat2.arrive(t)
        r = rows_of(t)
        h = jnp.dot(normed(full2[r, :], mod, 6), w1[...], preferred_element_type=F32)
        h = 0.5 * h * (1.0 + jnp.tanh(0.7978845608028654 * (h + 0.044715 * (h * h * h))))
        a3[r, 0:1024] = h.astype(BF)
        r3.share(t)

    def project3(t):
        @pl.when(t == 0)
        def _():
            ready(wou)

        r3.project(t)

    def put(t):
        r = rows_of(t)
        return pltpu.make_async_copy(res.at[r, :], out.at[r, :], ls.at[t])

    def back(t):
        r = rows_of(t)
        return rc(res.at[r, :], out.at[r, :], ss.at[t], sr.at[t], p.S)

    def finish3(t):
        r = rows_of(t)
        gate = mod[8:9, here]
        res[r, :] = (full2[r, here].astype(F32) + gate * r3.total(t)).astype(BF)

        @pl.when(p.c == p.zl)
        def _():
            put(t).start()

        @pl.when(p.c != p.zl)
        def _():
            back(t).start()

    def steps(*entries):
        def body(i, carry):
            for first, count, function in entries:

                @pl.when((i >= first) & (i < first + count))
                def _(t=i - first, function=function):
                    function(t)

            return carry

        lax.fori_loop(0, NC + FINISH3, body, 0)

    def twice(piece):
        def run(i):
            piece(2 * i)
            piece(2 * i + 1)

        return run

    steps(
        (0, 8, wtq.piece), (8, 4, wto.piece), (12, 8, twice(whi.piece)), (20, 8, twice(wou.piece)),
        (FINISH, NC, finish1), (ENTER, NC, enter1), (RELAY, NC, gat1.relay), (FAR, NC, gat1.far),
        (NEAR, NC, r1.near), (NEAR2, NC, r2.near), (NEAR3, NC, r3.near),
        (FINISH2, NC, finish2), (RELAY2, NC, gat2.relay), (FAR2, NC, gat2.far), (FINISH3, NC, finish3),
        (PROJECT, NC, project1), (PROJECT2, NC, project2), (PROJECT3, NC, project3),
        (0, NC, heads), (COMPUTE, NC, temporal), (COMPUTE2, NC, hidden),
    )

    def drain(t):
        for stage in (r1, r2, r3, gat1, gat2):
            stage.drain(t)
        each(15, lambda k: cross(k + 1, t).wait_send())

    each(NC, drain)
    for weights in (wso, wtq, wto, whi, wou):
        for d in range(2):
            weights.whole(d).wait_send()

    @pl.when(p.c == p.zl)
    def _():
        each(NC, lambda t: put(t).wait())

    @pl.when(p.c != p.zl)
    def _():
        each(NC, lambda t: back(t).wait())


def call(kernel, name, ident, ins, outs, scratch, limit, cost):
    return pl.pallas_call(
        kernel,
        name=name,
        out_shape=[jax.ShapeDtypeStruct(shape, BF) for shape, _ in outs],
        in_specs=ins,
        out_specs=[spec for _, spec in outs],
        scratch_shapes=scratch,
        compiler_params=pltpu.CompilerParams(
            collective_id=ident, has_side_effects=True, vmem_limit_bytes=limit << 20
        ),
        cost_estimate=pl.CostEstimate(flops=cost, bytes_accessed=1 << 24, transcendentals=0),
    )


def input_scratch():
    return [
        VM((T, D), BF), VM((T, D), BF), VM((D, 384), BF), VM((D, 384), BF),
        DMA((9, NC)), DMA((9, NC)), DMA((2,)), DMA((2,)), DMA((3,)), DMA((NC,)), DMA((NC,)), DMA((NC,)),
    ]


def tail_scratch():
    def reduce(width):
        return [VM((T, width), BF), VM((2, T, 128), BF), VM((2, T, 128), BF), VM((2, T, B), BF), VM((2, T, B), BF)]

    pair = [DMA((2,)), DMA((2,))]
    return (
        [VM((2, T, B), BF), VM((512, 1024), BF), VM((T, B), BF), VM((T, D), BF), VM((D, 384), BF), VM((D, 384), BF)]
        + [VM((512, 1024), BF), VM((T, D), BF), VM((D, 1024), BF), VM((D, 1024), BF), VM((T, B), BF), VM((T, 768), F32)]
        + reduce(512) + reduce(512) + reduce(2048)
        + [DMA((5, NC))] * 6 + [DMA((9, NC))] * 4
        + pair * 5 + [DMA((8,)), DMA((3,)), DMA((8,)), DMA((1,)), DMA((8,))]
        + [DMA((16, NC)), DMA((16, NC)), DMA((NC,)), DMA((NC,)), DMA((NC,))]
    )


def per_device(latent, mod, sqkv, so, tqkv, to, hw, ow):
    tokens = latent.reshape(16, 8, 8, B).transpose(1, 0, 2, 3).reshape(T, B)
    qkv, own = call(
        spatial_in, "spatial_in", 0, [ANY, INV, ANY], [((T, 768), INV), ((T, B), INV)], input_scratch(), 60, 10**10
    )(tokens, mod, sqkv)
    (out,) = call(
        tail, "tail", 1, [INV, INV, INV] + [ANY] * 5, [((T, B), ANY)], tail_scratch(), 60, 4 * 10**10
    )(qkv, own, mod, so, tqkv, to, hw, ow)
    return out.reshape(8, 16, 8, B).transpose(1, 0, 2, 3).reshape(16, 64, B)


def solution(mesh):
    in_specs = (
        P("seq", None, "head"), P(), P(None, None, "head"), P("head", None),
        P(None, None, "head"), P("head", None), P(None, "head"), P("head", None),
    )
    return jax.shard_map(
        per_device, mesh=mesh, in_specs=in_specs, out_specs=P(None, "seq", "head"), check_vma=False
    )
```

```python
import functools

import jax
import jax.numpy as jnp
from jax import lax
from jax.experimental import pallas as pl
from jax.experimental.pallas import tpu as pltpu
from jax.sharding import PartitionSpec as P

MESH = pl.DeviceIdType.MESH
BF = jnp.bfloat16
F32 = jnp.float32
T = 1024
D = 2048
B = 256
VM = pltpu.VMEM
ANY = pl.BlockSpec(memory_space=pltpu.MemorySpace.HBM)
INV = pl.BlockSpec(memory_space=pltpu.VMEM)


def rc(src, dst, ss, rs, dev):
    return pltpu.make_async_remote_copy(
        src_ref=src, dst_ref=dst, send_sem=ss, recv_sem=rs, device_id=dev, device_id_type=MESH
    )


class Place:
    def __init__(self):
        s, h = lax.axis_index("seq"), lax.axis_index("head")
        self.c, self.y, self.zh = lax.rem(s, 2), lax.rem(lax.div(s, 2), 4), lax.div(s, 8)
        self.x, self.zl = lax.div(h, 2), lax.rem(h, 2)
        self.z = self.zh * 2 + self.zl
        self.o = 1 - self.c
        self.row = (self.zh * 4 + self.y) * 2 + self.zl
        self.xr, self.xl, self.xf = [lax.rem(self.x + k, 4) for k in (1, 3, 2)]
        self.R = self.dev(self.xr, self.z, self.c)
        self.L = self.dev(self.xl, self.z, self.c)
        self.D = self.dev(self.x, self.z, self.o)
        self.U = self.dev(self.x, lax.rem(self.z + 1, 4), self.c)
        self.N = self.dev(self.x, lax.rem(self.z + 3, 4), self.c)
        self.S = ((self.zh * 4 + self.y) * 2 + self.o, self.x * 2 + 1 - self.zl)

    def dev(self, x, z, c):
        return ((lax.div(z, 2) * 4 + self.y) * 2 + c, x * 2 + lax.rem(z, 2))

    def row_dev(self, row):
        return (lax.div(row, 2) * 2 + self.c, self.x * 2 + lax.rem(row, 2))


def greet(devices):
    barrier = pltpu.get_barrier_semaphore()
    for device in devices:
        pl.semaphore_signal(barrier, inc=1, device_id=device, device_id_type=MESH)
    pl.semaphore_wait(barrier, len(devices))


def blk(x, c, width=B, off=0):
    return pl.ds(pl.multiple_of((x * 2 + c) * B + off, 128), width)


class Gather:
    KINDS = 9

    def __init__(self, p, full, rows, ss, rs):
        self.p, self.full, self.rows, self.ss, self.rs = p, full, rows, ss, rs
        x, c, o = p.x, p.c, p.o
        H = 128
        self.sent = [
            (blk(x, c), p.R), (blk(x, c), p.L), (blk(x, c), p.D),
            (blk(p.xl, c, H), p.R), (blk(p.xr, c, H, H), p.L),
            (blk(p.xl, c), p.D), (blk(p.xr, c), p.D),
            (blk(p.xf, c, H), p.D), (blk(p.xf, c, H, H), p.D),
        ]
        self.landed = [
            blk(p.xl, c), blk(p.xr, c), blk(x, o),
            blk(p.xf, c, H), blk(p.xf, c, H, H),
            blk(p.xl, o), blk(p.xr, o),
            blk(p.xf, o, H), blk(p.xf, o, H, H),
        ]

    def out(self, k, t):
        cols, dev = self.sent[k]
        ref = self.full.at[(*self.rows(t), cols)]
        return rc(ref, ref, self.ss.at[k, t], self.rs.at[k, t], dev)

    def got(self, k, t):
        ref = self.full.at[(*self.rows(t), self.landed[k])]
        rc(ref, ref, self.ss.at[k, t], self.rs.at[k, t], self.sent[k][1]).wait_recv()

    def own(self, t):
        for k in (0, 1, 2):
            self.out(k, t).start()

    def relay(self, t):
        self.got(0, t)
        self.out(3, t).start()
        self.out(5, t).start()
        self.got(1, t)
        self.out(4, t).start()
        self.out(6, t).start()

    def far(self, t):
        self.got(3, t)
        self.out(7, t).start()
        self.got(4, t)
        self.out(8, t).start()

    def arrive(self, t):
        for k in (2, 5, 6, 7, 8):
            self.got(k, t)

    def drain(self, t):
        for k in range(9):
            self.out(k, t).wait_send()


class Reduce:
    def __init__(self, p, ch, act, half, w, part, fs, fr, ns, nr, ss, rs):
        self.p, self.ch, self.act, self.half, self.w, self.part = p, ch, act, half, w, part
        self.fs, self.fr, self.ns, self.nr, self.ss, self.rs = fs, fr, ns, nr, ss, rs

    def r(self, t):
        return pl.ds(pl.multiple_of(t * self.ch, self.ch), self.ch)

    def copy(self, k, t):
        p, r = self.p, self.r(t)
        if k == 0:
            src, dst, dev = self.act.at[r, 0 : self.half], self.act.at[r, self.half : 2 * self.half], p.D
        elif k in (1, 2):
            src, dst, dev = self.fs.at[k - 1, r], self.fr.at[k - 1, r], (p.R, p.L)[k - 1]
        else:
            src, dst, dev = self.ns.at[k - 3, r], self.nr.at[k - 3, r], (p.R, p.L)[k - 3]
        return rc(src, dst, self.ss.at[k, t], self.rs.at[k, t], dev)

    def share(self, t):
        self.copy(0, t).start()

    def project(self, t):
        r = self.r(t)
        self.copy(0, t).wait_recv()
        out = jnp.dot(self.act[r, :], self.w[...], preferred_element_type=F32)
        self.fs[0, r] = out[:, 512:640].astype(BF)
        self.fs[1, r] = out[:, 640:768].astype(BF)
        self.copy(1, t).start()
        self.copy(2, t).start()
        self.part[r, 0:512] = out[:, 0:512]
        self.part[r, 512:768] = out[:, 768:1024]

    def near(self, t):
        r = self.r(t)
        self.copy(1, t).wait_recv()
        self.ns[0, r, 0:128] = (self.part[r, 256:384] + self.fr[0, r].astype(F32)).astype(BF)
        self.ns[0, r, 128:256] = self.part[r, 384:512].astype(BF)
        self.copy(3, t).start()
        self.copy(2, t).wait_recv()
        self.ns[1, r, 0:128] = self.part[r, 512:640].astype(BF)
        self.ns[1, r, 128:256] = (self.part[r, 640:768] + self.fr[1, r].astype(F32)).astype(BF)
        self.copy(4, t).start()

    def total(self, t):
        r = self.r(t)
        self.copy(3, t).wait_recv()
        self.copy(4, t).wait_recv()
        return self.part[r, 0:256] + self.nr[0, r].astype(F32) + self.nr[1, r].astype(F32)

    def drain(self, t):
        for k in range(5):
            self.copy(k, t).wait_send()


def normed(values, mod, row):
    v = values.astype(F32)
    v = v - jnp.mean(v, axis=-1, keepdims=True)
    v = v * lax.rsqrt(jnp.mean(v * v, axis=-1, keepdims=True) + 1e-06)
    return (v * (1.0 + mod[row + 1 : row + 2, :]) + mod[row : row + 1, :]).astype(BF)


def each(n, function):
    def body(i, carry):
        function(i)
        return carry

    lax.fori_loop(0, n, body, 0)


class QKV:
    def __init__(self, p, w, mine, theirs, ss, rs, ls):
        self.p, self.w, self.mine, self.theirs, self.ss, self.rs, self.ls = p, w, mine, theirs, ss, rs, ls
        self.half = pl.ds(pl.multiple_of(p.c * 128, 128), 128)

    def locals(self):
        return [
            pltpu.make_async_copy(self.w.at[j, :, self.half], self.mine.at[:, j * 128 : j * 128 + 128], self.ls.at[j])
            for j in range(3)
        ]

    def piece(self, i):
        for d, dev in enumerate((self.p.U, self.p.N)):
            rows = pl.ds(pl.multiple_of(d * 1024 + i * 128, 128), 128)
            for j in range(3):
                rc(
                    self.w.at[j, rows, self.half], self.theirs.at[rows, j * 128 : j * 128 + 128],
                    self.ss.at[d], self.rs.at[d], dev,
                ).start()

    def whole(self, d):
        ref = self.theirs.at[d * 1024 : d * 1024 + 1024, :]
        return rc(ref, ref, self.ss.at[d], self.rs.at[d], (self.p.U, self.p.N)[d])


class Out:
    def __init__(self, p, w, dst, rows, ss, rs, ls):
        self.p, self.w, self.dst, self.rows, self.ss, self.rs, self.ls = p, w, dst, rows, ss, rs, ls

    def src(self, g, j, first, count):
        start = (self.p.c, self.p.o)[g] * self.rows + first
        return self.w.at[pl.ds(pl.multiple_of(start, 128), count), blk(lax.rem(self.p.x + j, 4), self.p.c)]

    def locals(self):
        n = self.rows
        return [
            pltpu.make_async_copy(
                self.src(g, j, 0, n), self.dst.at[2 * g * n : 2 * g * n + n, j * B : j * B + B], self.ls.at[g * 4 + j]
            )
            for g in range(2)
            for j in range(4)
        ]

    def piece(self, i):
        n = self.rows
        per = n // 128
        j, first = lax.div(i, per), lax.rem(i, per) * 128
        for g, dev in enumerate((self.p.U, self.p.N)):
            rows = pl.ds(pl.multiple_of((2 * g + 1) * n + first, 128), 128)
            rc(
                self.src(g, j, first, 128), self.dst.at[rows, pl.ds(pl.multiple_of(j * B, B), B)],
                self.ss.at[g], self.rs.at[g], dev,
            ).start()

    def whole(self, g):
        n = self.rows
        ref = self.dst.at[(2 * g + 1) * n : (2 * g + 2) * n, :]
        return rc(ref, ref, self.ss.at[g], self.rs.at[g], (self.p.U, self.p.N)[g])


class Hidden:
    def __init__(self, p, w, dst, ss, rs, ls):
        self.p, self.w, self.dst, self.ss, self.rs, self.ls = p, w, dst, ss, rs, ls
        self.half = pl.ds(pl.multiple_of(p.c * 512, 512), 512)

    def locals(self):
        return [pltpu.make_async_copy(self.w.at[:, self.half], self.dst.at[:, 0:512], self.ls.at[0])]

    def piece(self, i):
        for d, dev in enumerate((self.p.U, self.p.N)):
            rows = pl.ds(pl.multiple_of(d * 1024 + i * 64, 64), 64)
            rc(
                self.w.at[rows, self.half], self.dst.at[rows, 512:1024], self.ss.at[d], self.rs.at[d], dev
            ).start()

    def whole(self, d):
        ref = self.dst.at[d * 1024 : d * 1024 + 1024, 512:1024]
        return rc(ref, ref, self.ss.at[d], self.rs.at[d], (self.p.U, self.p.N)[d])


def ready(weights):
    for d in range(2):
        weights.whole(d).wait_recv()
    for copy in weights.locals():
        copy.wait()


DMA = pltpu.SemaphoreType.DMA
NC, CH = 8, 128


def rows_of(t):
    return pl.ds(pl.multiple_of(t * CH, CH), CH)


def flat_rows(t):
    return (rows_of(t),)


def lanes(rows):
    return lax.broadcasted_iota(jnp.int32, (rows, 128), 1)


def head_pair(q, k, v, mask):
    lane = lanes(q.shape[0])
    outs = []
    for a in range(2):
        qa = jnp.where((lane < 64) == (a == 0), q, jnp.zeros_like(q))
        s = lax.dot_general(qa, k, (((1,), (1,)), ((), ())), preferred_element_type=F32)
        if mask is not None:
            s = jnp.where(mask, s, -1e30)
        e = jnp.exp(s - jnp.max(s, axis=-1, keepdims=True)).astype(BF)
        o = jnp.dot(e, v, preferred_element_type=F32)
        outs.append(o[:, 0:128] / o[:, 128:256])
    return jnp.where(lane < 64, outs[0], outs[1]).astype(BF)


PROJECT, NEAR, FINISH = 1, 3, 5
ENTER, RELAY, FAR, COMPUTE = 8, 10, 12, 13
PROJECT2, NEAR2, FINISH2 = 14, 16, 18
RELAY2, FAR2, COMPUTE2 = 20, 22, 23
PROJECT3, NEAR3, FINISH3 = 24, 26, 28


def block(
    latent, mod, sw, so, tw, to, hw, ow, out,
    qkv, full0, nrm, mine0, theirs0, g0, h0, zs, zr, zl_, ls0, ss0, sr0,
    vx, ws, one, full1, mine, theirs, wt, full2, w1, w2, res, part,
    a1, fs1, fr1, ns1, nr1, a2, fs2, fr2, ns2, nr2, a3, fs3, fr3, ns3, nr3,
    s1, v1, s2, v2, s3, v3, g1, h1, g2, h2,
    ps, pr, qs, qr, us, ur, hs, hr, os, orr, pl_, ql, ul, hl, ol, xs, xr, ls, ss, sr,
):
    p = Place()
    greet([p.L, p.R, p.D, p.S] + [p.row_dev(lax.rem(p.row + k, 16)) for k in range(1, 16)])
    here = blk(p.x, p.c)
    wsq = QKV(p, sw, mine0, theirs0, zs, zr, zl_)
    gat0 = Gather(p, full0, flat_rows, g0, h0)
    wso = Out(p, so, ws, 128, ps, pr, pl_)
    wtq = QKV(p, tw, mine, theirs, qs, qr, ql)
    wto = Out(p, to, wt, 128, us, ur, ul)
    whi = Hidden(p, hw, w1, hs, hr, hl)
    wou = Out(p, ow, w2, 512, os, orr, ol)
    r1 = Reduce(p, CH, a1, 256, ws, part, fs1, fr1, ns1, nr1, s1, v1)
    r2 = Reduce(p, CH, a2, 256, wt, part, fs2, fr2, ns2, nr2, s2, v2)
    r3 = Reduce(p, CH, a3, 1024, w2, part, fs3, fr3, ns3, nr3, s3, v3)
    gat1 = Gather(p, full1, flat_rows, g1, h1)
    gat2 = Gather(p, full2, flat_rows, g2, h2)

    def eight(t, row):
        return pl.ds(pl.multiple_of(t * CH + row * 8, 8), 8)

    def strip(t, row):
        return pl.ds(pl.multiple_of(row * 64 + t * 8, 8), 8)

    def keep(t):
        each(16, lambda k: pltpu.make_async_copy(latent.at[strip(t, k), :], full0.at[eight(t, k), here], ls0.at[t]).start())

    def kept(t):
        r = rows_of(t)
        return pltpu.make_async_copy(latent.at[r, :], full0.at[r, here], ls0.at[t])

    def swap(t):
        there = blk(p.x, p.o)
        each(
            16,
            lambda k: rc(
                latent.at[strip(t, k), :], full0.at[eight(t, k), there], ss0.at[t], sr0.at[t], p.S
            ).start(),
        )

    def swapped(t):
        r = rows_of(t)
        return rc(latent.at[r, :], full0.at[r, here], ss0.at[t], sr0.at[t], p.S)

    @pl.when(p.c == p.zl)
    def _():
        each(NC, keep)

    @pl.when(p.c != p.zl)
    def _():
        each(NC, swap)

    for copy in wsq.locals():
        copy.start()
    each(NC, wsq.piece)
    each(4, wso.piece)
    for weights in (wso, wtq, wto, whi, wou):
        for copy in weights.locals():
            copy.start()

    def first(t):
        @pl.when(p.c == p.zl)
        def _():
            kept(t).wait()

        @pl.when(p.c != p.zl)
        def _():
            swapped(t).wait_recv()

        gat0.own(t)

    def spatial(t):
        @pl.when(t == 0)
        def _():
            for copy in wsq.locals():
                copy.wait()

        gat0.arrive(t)
        r = rows_of(t)
        nrm[r, :] = normed(full0[r, :], mod, 0)
        qkv[r, 0:384] = jnp.dot(nrm[r, :], mine0[...], preferred_element_type=F32).astype(BF)

    def spatial_rest(t):
        @pl.when(t == 0)
        def _():
            for d in range(2):
                wsq.whole(d).wait_recv()

        r = rows_of(t)
        qkv[r, 384:768] = jnp.dot(nrm[r, :], theirs0[...], preferred_element_type=F32).astype(BF)

    def steps(total, *entries):
        def body(i, carry):
            for start, count, function in entries:

                @pl.when((i >= start) & (i < start + count))
                def _(t=i - start, function=function):
                    function(t)

            return carry

        lax.fori_loop(0, total, body, 0)

    steps(
        NC + 10,
        (0, NC, first), (2, NC, gat0.relay), (4, NC, gat0.far), (6, 8, wtq.piece), (6, NC, spatial), (10, NC, spatial_rest),
    )
    for pair in range(2):
        vx[pair, :, 0:128] = qkv[:, pair * 384 + 256 : pair * 384 + 384]
        vx[pair, :, 128:256] = jnp.ones((T, 128), BF)

    def heads(t):
        r = rows_of(t)
        for pair in range(2):
            base = pair * 384
            q = qkv[r, base : base + 128] * jnp.array(0.125, BF)
            a1[r, pair * 128 : pair * 128 + 128] = head_pair(q, qkv[:, base + 128 : base + 256], vx[pair], None)
        r1.share(t)

    def project1(t):
        @pl.when(t == 0)
        def _():
            ready(wso)

        r1.project(t)

    def cross(k, t):
        row = lax.rem(p.row + k, 16)
        return rc(one.at[eight(t, row), :], full1.at[eight(t, p.row), here], xs.at[k, t], xr.at[p.row, t], p.row_dev(row))

    def stay(t):
        return pltpu.make_async_copy(one.at[eight(t, p.row), :], full1.at[eight(t, p.row), here], xr.at[p.row, t])

    def finish1(t):
        r = rows_of(t)
        gate = mod[2:3, here]
        one[r, :] = (full0[r, here].astype(F32) + gate * r1.total(t)).astype(BF)
        each(15, lambda k: cross(k + 1, t).start())
        stay(t).start()

    def enter1(t):
        def arrived(k):
            row = lax.rem(p.row + k, 16)
            rc(
                one.at[eight(t, row), :], full1.at[eight(t, row), here], xs.at[k, t], xr.at[row, t], p.row_dev(row)
            ).wait_recv()

        each(15, lambda k: arrived(k + 1))
        stay(t).wait()
        gat1.own(t)

    i = lax.broadcasted_iota(jnp.int32, (CH, CH), 0)
    j = lax.broadcasted_iota(jnp.int32, (CH, CH), 1)
    same = lax.rem(i, 8) == lax.rem(j, 8)

    def temporal(t):
        @pl.when(t == 0)
        def _():
            ready(wtq)

        gat1.arrive(t)
        r = rows_of(t)
        n = normed(full1[r, :], mod, 3)
        for pair, w in enumerate((mine, theirs)):
            y = jnp.dot(n, w[...], preferred_element_type=F32).astype(BF)
            v = jnp.concatenate([y[:, 256:384], jnp.ones((CH, 128), BF)], axis=1)
            a2[r, pair * 128 : pair * 128 + 128] = head_pair(
                y[:, 0:128] * jnp.array(0.125, BF), y[:, 128:256], v, same
            )
        r2.share(t)

    def project2(t):
        @pl.when(t == 0)
        def _():
            ready(wto)

        r2.project(t)

    def finish2(t):
        r = rows_of(t)
        gate = mod[5:6, here]
        full2[r, here] = (full1[r, here].astype(F32) + gate * r2.total(t)).astype(BF)
        gat2.own(t)

    def hidden(t):
        @pl.when(t == 0)
        def _():
            ready(whi)

        gat2.arrive(t)
        r = rows_of(t)
        h = jnp.dot(normed(full2[r, :], mod, 6), w1[...], preferred_element_type=F32)
        h = 0.5 * h * (1.0 + jnp.tanh(0.7978845608028654 * (h + 0.044715 * (h * h * h))))
        a3[r, 0:1024] = h.astype(BF)
        r3.share(t)

    def project3(t):
        @pl.when(t == 0)
        def _():
            ready(wou)

        r3.project(t)

    def put(t):
        each(16, lambda k: pltpu.make_async_copy(res.at[eight(t, k), :], out.at[strip(t, k), :], ls.at[t]).start())

    def putted(t):
        r = rows_of(t)
        return pltpu.make_async_copy(res.at[r, :], out.at[r, :], ls.at[t])

    def back(t):
        each(16, lambda k: rc(res.at[eight(t, k), :], out.at[strip(t, k), :], ss.at[t], sr.at[t], p.S).start())

    def backed(t):
        r = rows_of(t)
        return rc(res.at[r, :], out.at[r, :], ss.at[t], sr.at[t], p.S)

    def finish3(t):
        r = rows_of(t)
        gate = mod[8:9, here]
        res[r, :] = (full2[r, here].astype(F32) + gate * r3.total(t)).astype(BF)

        @pl.when(p.c == p.zl)
        def _():
            put(t)

        @pl.when(p.c != p.zl)
        def _():
            back(t)

    def twice(piece):
        def run(i):
            piece(2 * i)
            piece(2 * i + 1)

        return run

    steps(
        NC + FINISH3,
        (0, 4, wto.piece), (2, 3, twice(whi.piece)), (5, 10, lambda i: whi.piece(i + 6)), (15, 8, twice(wou.piece)),
        (FINISH, NC, finish1), (ENTER, NC, enter1), (RELAY, NC, gat1.relay), (FAR, NC, gat1.far),
        (NEAR, NC, r1.near), (NEAR2, NC, r2.near), (NEAR3, NC, r3.near),
        (FINISH2, NC, finish2), (RELAY2, NC, gat2.relay), (FAR2, NC, gat2.far), (FINISH3, NC, finish3),
        (PROJECT, NC, project1), (PROJECT2, NC, project2), (PROJECT3, NC, project3),
        (0, NC, heads), (COMPUTE, NC, temporal), (COMPUTE2, NC, hidden),
    )

    def drain(t):
        for stage in (r1, r2, r3, gat0, gat1, gat2):
            stage.drain(t)
        each(15, lambda k: cross(k + 1, t).wait_send())

    each(NC, drain)
    for weights in (wsq, wso, wtq, wto, whi, wou):
        for d in range(2):
            weights.whole(d).wait_send()

    @pl.when(p.c != p.zl)
    def _():
        each(NC, lambda t: swapped(t).wait_send())

    @pl.when(p.c == p.zl)
    def _():
        each(NC, lambda t: putted(t).wait())

    @pl.when(p.c != p.zl)
    def _():
        each(NC, lambda t: backed(t).wait())


def call(kernel, name, ident, ins, outs, scratch, limit, cost):
    return pl.pallas_call(
        kernel,
        name=name,
        out_shape=[jax.ShapeDtypeStruct(shape, BF) for shape, _ in outs],
        in_specs=ins,
        out_specs=[spec for _, spec in outs],
        scratch_shapes=scratch,
        compiler_params=pltpu.CompilerParams(
            collective_id=ident, has_side_effects=True, vmem_limit_bytes=limit << 20
        ),
        cost_estimate=pl.CostEstimate(flops=cost, bytes_accessed=1 << 24, transcendentals=0),
    )


def input_scratch():
    return [
        VM((T, 768), BF), VM((T, D), BF), VM((T, D), BF), VM((D, 384), BF), VM((D, 384), BF),
        DMA((9, NC)), DMA((9, NC)), DMA((2,)), DMA((2,)), DMA((3,)), DMA((NC,)), DMA((NC,)), DMA((NC,)),
    ]


def tail_scratch():
    def reduce(width):
        return [VM((T, width), BF), VM((2, T, 128), BF), VM((2, T, 128), BF), VM((2, T, B), BF), VM((2, T, B), BF)]

    pair = [DMA((2,)), DMA((2,))]
    return (
        [VM((2, T, B), BF), VM((512, 1024), BF), VM((T, B), BF), VM((T, D), BF), VM((D, 384), BF), VM((D, 384), BF)]
        + [VM((512, 1024), BF), VM((T, D), BF), VM((D, 1024), BF), VM((D, 1024), BF), VM((T, B), BF), VM((T, 768), F32)]
        + reduce(512) + reduce(512) + reduce(2048)
        + [DMA((5, NC))] * 6 + [DMA((9, NC))] * 4
        + pair * 5 + [DMA((8,)), DMA((3,)), DMA((8,)), DMA((1,)), DMA((8,))]
        + [DMA((16, NC)), DMA((16, NC)), DMA((NC,)), DMA((NC,)), DMA((NC,))]
    )


def per_device(latent, mod, *weights):
    (out,) = call(
        block, "block", 0, [ANY, INV] + [ANY] * 6, [((T, B), ANY)], input_scratch() + tail_scratch(), 63, 4 * 10**10
    )(latent.reshape(T, B), mod, *weights)
    return out.reshape(16, 64, B)


def solution(mesh):
    in_specs = (
        P("seq", None, "head"), P(), P(None, None, "head"), P("head", None),
        P(None, None, "head"), P("head", None), P(None, "head"), P("head", None),
    )
    return jax.shard_map(
        per_device, mesh=mesh, in_specs=in_specs, out_specs=P(None, "seq", "head"), check_vma=False
    )
```

```python
import functools

import jax
import jax.numpy as jnp
from jax import lax
from jax.experimental import pallas as pl
from jax.experimental.pallas import tpu as pltpu
from jax.sharding import PartitionSpec as P

MESH = pl.DeviceIdType.MESH
BF = jnp.bfloat16
F32 = jnp.float32
T = 1024
D = 2048
B = 256
VM = pltpu.VMEM
ANY = pl.BlockSpec(memory_space=pltpu.MemorySpace.HBM)
INV = pl.BlockSpec(memory_space=pltpu.VMEM)


def rc(src, dst, ss, rs, dev):
    return pltpu.make_async_remote_copy(
        src_ref=src, dst_ref=dst, send_sem=ss, recv_sem=rs, device_id=dev, device_id_type=MESH
    )


class Place:
    def __init__(self):
        s, h = lax.axis_index("seq"), lax.axis_index("head")
        self.c, self.y, self.zh = lax.rem(s, 2), lax.rem(lax.div(s, 2), 4), lax.div(s, 8)
        self.x, self.zl = lax.div(h, 2), lax.rem(h, 2)
        self.z = self.zh * 2 + self.zl
        self.o = 1 - self.c
        self.row = (self.zh * 4 + self.y) * 2 + self.zl
        self.xr, self.xl, self.xf = [lax.rem(self.x + k, 4) for k in (1, 3, 2)]
        self.R = self.dev(self.xr, self.z, self.c)
        self.L = self.dev(self.xl, self.z, self.c)
        self.D = self.dev(self.x, self.z, self.o)
        self.U = self.dev(self.x, lax.rem(self.z + 1, 4), self.c)
        self.N = self.dev(self.x, lax.rem(self.z + 3, 4), self.c)
        self.S = ((self.zh * 4 + self.y) * 2 + self.o, self.x * 2 + 1 - self.zl)

    def dev(self, x, z, c):
        return ((lax.div(z, 2) * 4 + self.y) * 2 + c, x * 2 + lax.rem(z, 2))

    def row_dev(self, row):
        return (lax.div(row, 2) * 2 + self.c, self.x * 2 + lax.rem(row, 2))


def greet(devices):
    barrier = pltpu.get_barrier_semaphore()
    for device in devices:
        pl.semaphore_signal(barrier, inc=1, device_id=device, device_id_type=MESH)
    pl.semaphore_wait(barrier, len(devices))


def blk(x, c, width=B, off=0):
    return pl.ds(pl.multiple_of((x * 2 + c) * B + off, 128), width)


class Gather:
    KINDS = 9

    def __init__(self, p, full, rows, ss, rs):
        self.p, self.full, self.rows, self.ss, self.rs = p, full, rows, ss, rs
        x, c, o = p.x, p.c, p.o
        H = 128
        self.sent = [
            (blk(x, c), p.R), (blk(x, c), p.L), (blk(x, c), p.D),
            (blk(p.xl, c, H), p.R), (blk(p.xr, c, H, H), p.L),
            (blk(p.xl, c), p.D), (blk(p.xr, c), p.D),
            (blk(p.xf, c, H), p.D), (blk(p.xf, c, H, H), p.D),
        ]
        self.landed = [
            blk(p.xl, c), blk(p.xr, c), blk(x, o),
            blk(p.xf, c, H), blk(p.xf, c, H, H),
            blk(p.xl, o), blk(p.xr, o),
            blk(p.xf, o, H), blk(p.xf, o, H, H),
        ]

    def out(self, k, t):
        cols, dev = self.sent[k]
        ref = self.full.at[(*self.rows(t), cols)]
        return rc(ref, ref, self.ss.at[k, t], self.rs.at[k, t], dev)

    def got(self, k, t):
        ref = self.full.at[(*self.rows(t), self.landed[k])]
        rc(ref, ref, self.ss.at[k, t], self.rs.at[k, t], self.sent[k][1]).wait_recv()

    def own(self, t):
        for k in (0, 1, 2):
            self.out(k, t).start()

    def relay(self, t):
        self.got(0, t)
        self.out(3, t).start()
        self.out(5, t).start()
        self.got(1, t)
        self.out(4, t).start()
        self.out(6, t).start()

    def far(self, t):
        self.got(3, t)
        self.out(7, t).start()
        self.got(4, t)
        self.out(8, t).start()

    def arrive(self, t):
        for k in (2, 5, 6, 7, 8):
            self.got(k, t)

    def drain(self, t):
        for k in range(9):
            self.out(k, t).wait_send()


class Reduce:
    def __init__(self, p, ch, act, half, w, part, fs, fr, ns, nr, ss, rs):
        self.p, self.ch, self.act, self.half, self.w, self.part = p, ch, act, half, w, part
        self.fs, self.fr, self.ns, self.nr, self.ss, self.rs = fs, fr, ns, nr, ss, rs

    def r(self, t):
        return pl.ds(pl.multiple_of(t * self.ch, self.ch), self.ch)

    def copy(self, k, t):
        p, r = self.p, self.r(t)
        if k == 0:
            src, dst, dev = self.act.at[r, 0 : self.half], self.act.at[r, self.half : 2 * self.half], p.D
        elif k in (1, 2):
            src, dst, dev = self.fs.at[k - 1, r], self.fr.at[k - 1, r], (p.R, p.L)[k - 1]
        else:
            src, dst, dev = self.ns.at[k - 3, r], self.nr.at[k - 3, r], (p.R, p.L)[k - 3]
        return rc(src, dst, self.ss.at[k, t], self.rs.at[k, t], dev)

    def share(self, t):
        self.copy(0, t).start()

    def project(self, t):
        r = self.r(t)
        self.copy(0, t).wait_recv()
        out = jnp.dot(self.act[r, :], self.w[...], preferred_element_type=F32)
        self.fs[0, r] = out[:, 512:640].astype(BF)
        self.fs[1, r] = out[:, 640:768].astype(BF)
        self.copy(1, t).start()
        self.copy(2, t).start()
        self.part[r, 0:512] = out[:, 0:512]
        self.part[r, 512:768] = out[:, 768:1024]

    def near(self, t):
        r = self.r(t)
        self.copy(1, t).wait_recv()
        self.ns[0, r, 0:128] = (self.part[r, 256:384] + self.fr[0, r].astype(F32)).astype(BF)
        self.ns[0, r, 128:256] = self.part[r, 384:512].astype(BF)
        self.copy(3, t).start()
        self.copy(2, t).wait_recv()
        self.ns[1, r, 0:128] = self.part[r, 512:640].astype(BF)
        self.ns[1, r, 128:256] = (self.part[r, 640:768] + self.fr[1, r].astype(F32)).astype(BF)
        self.copy(4, t).start()

    def total(self, t):
        r = self.r(t)
        self.copy(3, t).wait_recv()
        self.copy(4, t).wait_recv()
        return self.part[r, 0:256] + self.nr[0, r].astype(F32) + self.nr[1, r].astype(F32)

    def drain(self, t):
        for k in range(5):
            self.copy(k, t).wait_send()


def normed(values, mod, row):
    v = values.astype(F32)
    v = v - jnp.mean(v, axis=-1, keepdims=True)
    v = v * lax.rsqrt(jnp.mean(v * v, axis=-1, keepdims=True) + 1e-06)
    return (v * (1.0 + mod[row + 1 : row + 2, :]) + mod[row : row + 1, :]).astype(BF)


def each(n, function):
    def body(i, carry):
        function(i)
        return carry

    lax.fori_loop(0, n, body, 0)


class QKV:
    def __init__(self, p, w, mine, theirs, ss, rs, ls):
        self.p, self.w, self.mine, self.theirs, self.ss, self.rs, self.ls = p, w, mine, theirs, ss, rs, ls
        self.half = pl.ds(pl.multiple_of(p.c * 128, 128), 128)

    def locals(self):
        return [
            pltpu.make_async_copy(self.w.at[j, :, self.half], self.mine.at[:, j * 128 : j * 128 + 128], self.ls.at[j])
            for j in range(3)
        ]

    def piece(self, i):
        for d, dev in enumerate((self.p.U, self.p.N)):
            rows = pl.ds(pl.multiple_of(d * 1024 + i * 128, 128), 128)
            for j in range(3):
                rc(
                    self.w.at[j, rows, self.half], self.theirs.at[rows, j * 128 : j * 128 + 128],
                    self.ss.at[d], self.rs.at[d], dev,
                ).start()

    def whole(self, d):
        ref = self.theirs.at[d * 1024 : d * 1024 + 1024, :]
        return rc(ref, ref, self.ss.at[d], self.rs.at[d], (self.p.U, self.p.N)[d])


class Out:
    def __init__(self, p, w, dst, rows, ss, rs, ls):
        self.p, self.w, self.dst, self.rows, self.ss, self.rs, self.ls = p, w, dst, rows, ss, rs, ls

    def src(self, g, j, first, count):
        start = (self.p.c, self.p.o)[g] * self.rows + first
        return self.w.at[pl.ds(pl.multiple_of(start, 128), count), blk(lax.rem(self.p.x + j, 4), self.p.c)]

    def locals(self):
        n = self.rows
        return [
            pltpu.make_async_copy(
                self.src(g, j, 0, n), self.dst.at[2 * g * n : 2 * g * n + n, j * B : j * B + B], self.ls.at[g * 4 + j]
            )
            for g in range(2)
            for j in range(4)
        ]

    def piece(self, i):
        n = self.rows
        per = n // 128
        j, first = lax.div(i, per), lax.rem(i, per) * 128
        for g, dev in enumerate((self.p.U, self.p.N)):
            rows = pl.ds(pl.multiple_of((2 * g + 1) * n + first, 128), 128)
            rc(
                self.src(g, j, first, 128), self.dst.at[rows, pl.ds(pl.multiple_of(j * B, B), B)],
                self.ss.at[g], self.rs.at[g], dev,
            ).start()

    def whole(self, g):
        n = self.rows
        ref = self.dst.at[(2 * g + 1) * n : (2 * g + 2) * n, :]
        return rc(ref, ref, self.ss.at[g], self.rs.at[g], (self.p.U, self.p.N)[g])


class Hidden:
    def __init__(self, p, w, dst, ss, rs, ls):
        self.p, self.w, self.dst, self.ss, self.rs, self.ls = p, w, dst, ss, rs, ls
        self.half = pl.ds(pl.multiple_of(p.c * 512, 512), 512)

    def locals(self):
        return [pltpu.make_async_copy(self.w.at[:, self.half], self.dst.at[:, 0:512], self.ls.at[0])]

    def piece(self, i):
        for d, dev in enumerate((self.p.U, self.p.N)):
            rows = pl.ds(pl.multiple_of(d * 1024 + i * 64, 64), 64)
            rc(
                self.w.at[rows, self.half], self.dst.at[rows, 512:1024], self.ss.at[d], self.rs.at[d], dev
            ).start()

    def whole(self, d):
        ref = self.dst.at[d * 1024 : d * 1024 + 1024, 512:1024]
        return rc(ref, ref, self.ss.at[d], self.rs.at[d], (self.p.U, self.p.N)[d])


def ready(weights):
    for d in range(2):
        weights.whole(d).wait_recv()
    for copy in weights.locals():
        copy.wait()


DMA = pltpu.SemaphoreType.DMA
NC, CH = 8, 128


def rows_of(t):
    return pl.ds(pl.multiple_of(t * CH, CH), CH)


def flat_rows(t):
    return (rows_of(t),)


def lanes(rows):
    return lax.broadcasted_iota(jnp.int32, (rows, 128), 1)


def head_pair(q, k, v, mask):
    lane = lanes(q.shape[0])
    outs = []
    for a in range(2):
        qa = jnp.where((lane < 64) == (a == 0), q, jnp.zeros_like(q))
        s = lax.dot_general(qa, k, (((1,), (1,)), ((), ())), preferred_element_type=F32)
        if mask is not None:
            s = jnp.where(mask, s, -1e30)
        e = jnp.exp(s - jnp.max(s, axis=-1, keepdims=True)).astype(BF)
        o = jnp.dot(e, v, preferred_element_type=F32)
        outs.append(o[:, 0:128] / o[:, 128:256])
    return jnp.where(lane < 64, outs[0], outs[1]).astype(BF)


PROJECT, NEAR, FINISH = 1, 3, 5
ENTER, RELAY, FAR, COMPUTE = 8, 10, 12, 13
PROJECT2, NEAR2, FINISH2 = 14, 16, 18
RELAY2, FAR2, COMPUTE2 = 20, 22, 23
PROJECT3, NEAR3, FINISH3 = 24, 26, 28
PLAN = ((1, 4, 1), (5, 4, 1), (9, 4, 2), (13, 10, 2))


def block(
    latent, mod, sw, so, tw, to, hw, ow, out,
    qkv, full0, nrm, mine0, theirs0, g0, h0, zs, zr, zl_, ls0, ss0, sr0,
    vx, ws, one, full1, mine, theirs, wt, full2, w1, w2, res, part,
    a1, fs1, fr1, ns1, nr1, a2, fs2, fr2, ns2, nr2, a3, fs3, fr3, ns3, nr3,
    s1, v1, s2, v2, s3, v3, g1, h1, g2, h2,
    ps, pr, qs, qr, us, ur, hs, hr, os, orr, pl_, ql, ul, hl, ol, xs, xr, ls, ss, sr,
):
    p = Place()
    greet([p.L, p.R, p.D, p.S] + [p.row_dev(lax.rem(p.row + k, 16)) for k in range(1, 16)])
    here = blk(p.x, p.c)
    wsq = QKV(p, sw, mine0, theirs0, zs, zr, zl_)
    gat0 = Gather(p, full0, flat_rows, g0, h0)
    wso = Out(p, so, ws, 128, ps, pr, pl_)
    wtq = QKV(p, tw, mine, theirs, qs, qr, ql)
    wto = Out(p, to, wt, 128, us, ur, ul)
    whi = Hidden(p, hw, w1, hs, hr, hl)
    wou = Out(p, ow, w2, 512, os, orr, ol)
    r1 = Reduce(p, CH, a1, 256, ws, part, fs1, fr1, ns1, nr1, s1, v1)
    r2 = Reduce(p, CH, a2, 256, wt, part, fs2, fr2, ns2, nr2, s2, v2)
    r3 = Reduce(p, CH, a3, 1024, w2, part, fs3, fr3, ns3, nr3, s3, v3)
    gat1 = Gather(p, full1, flat_rows, g1, h1)
    gat2 = Gather(p, full2, flat_rows, g2, h2)

    def eight(t, row):
        return pl.ds(pl.multiple_of(t * CH + row * 8, 8), 8)

    def strip(t, row):
        return pl.ds(pl.multiple_of(row * 64 + t * 8, 8), 8)

    def keep(t):
        each(16, lambda k: pltpu.make_async_copy(latent.at[strip(t, k), :], full0.at[eight(t, k), here], ls0.at[t]).start())

    def kept(t):
        r = rows_of(t)
        return pltpu.make_async_copy(latent.at[r, :], full0.at[r, here], ls0.at[t])

    def swap(t):
        there = blk(p.x, p.o)
        each(
            16,
            lambda k: rc(
                latent.at[strip(t, k), :], full0.at[eight(t, k), there], ss0.at[t], sr0.at[t], p.S
            ).start(),
        )

    def swapped(t):
        r = rows_of(t)
        return rc(latent.at[r, :], full0.at[r, here], ss0.at[t], sr0.at[t], p.S)

    @pl.when(p.c == p.zl)
    def _():
        each(NC, keep)

    @pl.when(p.c != p.zl)
    def _():
        each(NC, swap)

    for copy in wsq.locals():
        copy.start()
    each(NC, wsq.piece)
    each(4, wso.piece)
    for weights in (wso, wtq, wto, whi, wou):
        for copy in weights.locals():
            copy.start()

    def first(t):
        @pl.when(p.c == p.zl)
        def _():
            kept(t).wait()

        @pl.when(p.c != p.zl)
        def _():
            swapped(t).wait_recv()

        gat0.own(t)

    def spatial(t):
        @pl.when(t == 0)
        def _():
            for copy in wsq.locals():
                copy.wait()

        gat0.arrive(t)
        r = rows_of(t)
        nrm[r, :] = normed(full0[r, :], mod, 0)
        qkv[r, 0:384] = jnp.dot(nrm[r, :], mine0[...], preferred_element_type=F32).astype(BF)

    def spatial_rest(t):
        @pl.when(t == 0)
        def _():
            for d in range(2):
                wsq.whole(d).wait_recv()

        r = rows_of(t)
        qkv[r, 384:768] = jnp.dot(nrm[r, :], theirs0[...], preferred_element_type=F32).astype(BF)

    def steps(total, *entries):
        def body(i, carry):
            for start, count, function in entries:

                @pl.when((i >= start) & (i < start + count))
                def _(t=i - start, function=function):
                    function(t)

            return carry

        lax.fori_loop(0, total, body, 0)

    steps(
        NC + 10,
        (0, NC, first), (2, NC, gat0.relay), (4, NC, gat0.far), (6, 8, wtq.piece), (6, NC, spatial), (10, NC, spatial_rest),
    )
    for pair in range(2):
        vx[pair, :, 0:128] = qkv[:, pair * 384 + 256 : pair * 384 + 384]
        vx[pair, :, 128:256] = jnp.ones((T, 128), BF)

    def heads(t):
        r = rows_of(t)
        for pair in range(2):
            base = pair * 384
            q = qkv[r, base : base + 128] * jnp.array(0.125, BF)
            a1[r, pair * 128 : pair * 128 + 128] = head_pair(q, qkv[:, base + 128 : base + 256], vx[pair], None)
        r1.share(t)

    def project1(t):
        @pl.when(t == 0)
        def _():
            ready(wso)

        r1.project(t)

    def cross(k, t):
        row = lax.rem(p.row + k, 16)
        return rc(one.at[eight(t, row), :], full1.at[eight(t, p.row), here], xs.at[k, t], xr.at[p.row, t], p.row_dev(row))

    def stay(t):
        return pltpu.make_async_copy(one.at[eight(t, p.row), :], full1.at[eight(t, p.row), here], xr.at[p.row, t])

    def finish1(t):
        r = rows_of(t)
        gate = mod[2:3, here]
        one[r, :] = (full0[r, here].astype(F32) + gate * r1.total(t)).astype(BF)
        each(15, lambda k: cross(k + 1, t).start())
        stay(t).start()

    def enter1(t):
        def arrived(k):
            row = lax.rem(p.row + k, 16)
            rc(
                one.at[eight(t, row), :], full1.at[eight(t, row), here], xs.at[k, t], xr.at[row, t], p.row_dev(row)
            ).wait_recv()

        each(15, lambda k: arrived(k + 1))
        stay(t).wait()
        gat1.own(t)

    i = lax.broadcasted_iota(jnp.int32, (CH, CH), 0)
    j = lax.broadcasted_iota(jnp.int32, (CH, CH), 1)
    same = lax.rem(i, 8) == lax.rem(j, 8)

    def temporal(t):
        @pl.when(t == 0)
        def _():
            ready(wtq)

        gat1.arrive(t)
        r = rows_of(t)
        n = normed(full1[r, :], mod, 3)
        for pair, w in enumerate((mine, theirs)):
            y = jnp.dot(n, w[...], preferred_element_type=F32).astype(BF)
            v = jnp.concatenate([y[:, 256:384], jnp.ones((CH, 128), BF)], axis=1)
            a2[r, pair * 128 : pair * 128 + 128] = head_pair(
                y[:, 0:128] * jnp.array(0.125, BF), y[:, 128:256], v, same
            )
        r2.share(t)

    def project2(t):
        @pl.when(t == 0)
        def _():
            ready(wto)

        r2.project(t)

    def finish2(t):
        r = rows_of(t)
        gate = mod[5:6, here]
        full2[r, here] = (full1[r, here].astype(F32) + gate * r2.total(t)).astype(BF)
        gat2.own(t)

    def hidden(t):
        @pl.when(t == 0)
        def _():
            ready(whi)

        gat2.arrive(t)
        r = rows_of(t)
        h = jnp.dot(normed(full2[r, :], mod, 6), w1[...], preferred_element_type=F32)
        h = 0.5 * h * (1.0 + jnp.tanh(0.7978845608028654 * (h + 0.044715 * (h * h * h))))
        a3[r, 0:1024] = h.astype(BF)
        r3.share(t)

    def project3(t):
        @pl.when(t == 0)
        def _():
            ready(wou)

        r3.project(t)

    def put(t):
        each(16, lambda k: pltpu.make_async_copy(res.at[eight(t, k), :], out.at[strip(t, k), :], ls.at[t]).start())

    def putted(t):
        r = rows_of(t)
        return pltpu.make_async_copy(res.at[r, :], out.at[r, :], ls.at[t])

    def back(t):
        each(16, lambda k: rc(res.at[eight(t, k), :], out.at[strip(t, k), :], ss.at[t], sr.at[t], p.S).start())

    def backed(t):
        r = rows_of(t)
        return rc(res.at[r, :], out.at[r, :], ss.at[t], sr.at[t], p.S)

    def finish3(t):
        r = rows_of(t)
        gate = mod[8:9, here]
        res[r, :] = (full2[r, here].astype(F32) + gate * r3.total(t)).astype(BF)

        @pl.when(p.c == p.zl)
        def _():
            put(t)

        @pl.when(p.c != p.zl)
        def _():
            back(t)

    def pace(plan):
        order = [(wto, n) for n in range(4)] + [(whi, n) for n in range(16)] + [(wou, n) for n in range(16)]
        runs = []
        for start, count, rate in plan:
            for step in range(start, start + count):
                for weights, n in order[:rate]:
                    last = runs[-1] if runs else None
                    if last and last[0] is weights and last[2] == rate and (n - last[3]) // rate == step - last[1]:
                        last[4] = n + 1
                    else:
                        runs.append([weights, step, rate, n, n + 1])
                order = order[rate:]
        assert not order

        def entry(weights, step, rate, low, high):
            def run(i):
                for k in range(rate):
                    n = low + rate * i + k
                    if (high - low) % rate == 0:
                        weights.piece(n)
                    else:

                        @pl.when(n < high)
                        def _(n=n):
                            weights.piece(n)

            return step, -(-(high - low) // rate), run

        return [entry(*run) for run in runs]

    steps(
        NC + FINISH3,
        *pace(PLAN),
        (FINISH, NC, finish1), (ENTER, NC, enter1), (RELAY, NC, gat1.relay), (FAR, NC, gat1.far),
        (NEAR, NC, r1.near), (NEAR2, NC, r2.near), (NEAR3, NC, r3.near),
        (FINISH2, NC, finish2), (RELAY2, NC, gat2.relay), (FAR2, NC, gat2.far), (FINISH3, NC, finish3),
        (PROJECT, NC, project1), (PROJECT2, NC, project2), (PROJECT3, NC, project3),
        (0, NC, heads), (COMPUTE, NC, temporal), (COMPUTE2, NC, hidden),
    )

    def drain(t):
        for stage in (r1, r2, r3, gat0, gat1, gat2):
            stage.drain(t)
        each(15, lambda k: cross(k + 1, t).wait_send())

    each(NC, drain)
    for weights in (wsq, wso, wtq, wto, whi, wou):
        for d in range(2):
            weights.whole(d).wait_send()

    @pl.when(p.c != p.zl)
    def _():
        each(NC, lambda t: swapped(t).wait_send())

    @pl.when(p.c == p.zl)
    def _():
        each(NC, lambda t: putted(t).wait())

    @pl.when(p.c != p.zl)
    def _():
        each(NC, lambda t: backed(t).wait())


def call(kernel, name, ident, ins, outs, scratch, limit, cost):
    return pl.pallas_call(
        kernel,
        name=name,
        out_shape=[jax.ShapeDtypeStruct(shape, BF) for shape, _ in outs],
        in_specs=ins,
        out_specs=[spec for _, spec in outs],
        scratch_shapes=scratch,
        compiler_params=pltpu.CompilerParams(
            collective_id=ident, has_side_effects=True, vmem_limit_bytes=limit << 20
        ),
        cost_estimate=pl.CostEstimate(flops=cost, bytes_accessed=1 << 24, transcendentals=0),
    )


def input_scratch():
    return [
        VM((T, 768), BF), VM((T, D), BF), VM((T, D), BF), VM((D, 384), BF), VM((D, 384), BF),
        DMA((9, NC)), DMA((9, NC)), DMA((2,)), DMA((2,)), DMA((3,)), DMA((NC,)), DMA((NC,)), DMA((NC,)),
    ]


def tail_scratch():
    def reduce(width):
        return [VM((T, width), BF), VM((2, T, 128), BF), VM((2, T, 128), BF), VM((2, T, B), BF), VM((2, T, B), BF)]

    pair = [DMA((2,)), DMA((2,))]
    return (
        [VM((2, T, B), BF), VM((512, 1024), BF), VM((T, B), BF), VM((T, D), BF), VM((D, 384), BF), VM((D, 384), BF)]
        + [VM((512, 1024), BF), VM((T, D), BF), VM((D, 1024), BF), VM((D, 1024), BF), VM((T, B), BF), VM((T, 768), F32)]
        + reduce(512) + reduce(512) + reduce(2048)
        + [DMA((5, NC))] * 6 + [DMA((9, NC))] * 4
        + pair * 5 + [DMA((8,)), DMA((3,)), DMA((8,)), DMA((1,)), DMA((8,))]
        + [DMA((16, NC)), DMA((16, NC)), DMA((NC,)), DMA((NC,)), DMA((NC,))]
    )


def per_device(latent, mod, *weights):
    (out,) = call(
        block, "block", 0, [ANY, INV] + [ANY] * 6, [((T, B), ANY)], input_scratch() + tail_scratch(), 63, 4 * 10**10
    )(latent.reshape(T, B), mod, *weights)
    return out.reshape(16, 64, B)


def solution(mesh):
    in_specs = (
        P("seq", None, "head"), P(), P(None, None, "head"), P("head", None),
        P(None, None, "head"), P("head", None), P(None, "head"), P("head", None),
    )
    return jax.shard_map(
        per_device, mesh=mesh, in_specs=in_specs, out_specs=P(None, "seq", "head"), check_vma=False
    )
```

```python
import functools

import jax
import jax.numpy as jnp
from jax import lax
from jax.experimental import pallas as pl
from jax.experimental.pallas import tpu as pltpu
from jax.sharding import PartitionSpec as P

MESH = pl.DeviceIdType.MESH
BF = jnp.bfloat16
F32 = jnp.float32
T = 1024
D = 2048
B = 256
VM = pltpu.VMEM
ANY = pl.BlockSpec(memory_space=pltpu.MemorySpace.HBM)
INV = pl.BlockSpec(memory_space=pltpu.VMEM)


def rc(src, dst, ss, rs, dev):
    return pltpu.make_async_remote_copy(
        src_ref=src, dst_ref=dst, send_sem=ss, recv_sem=rs, device_id=dev, device_id_type=MESH
    )


class Place:
    def __init__(self):
        s, h = lax.axis_index("seq"), lax.axis_index("head")
        self.c, self.y, self.zh = lax.rem(s, 2), lax.rem(lax.div(s, 2), 4), lax.div(s, 8)
        self.x, self.zl = lax.div(h, 2), lax.rem(h, 2)
        self.z = self.zh * 2 + self.zl
        self.o = 1 - self.c
        self.row = (self.zh * 4 + self.y) * 2 + self.zl
        self.xr, self.xl, self.xf = [lax.rem(self.x + k, 4) for k in (1, 3, 2)]
        self.R = self.dev(self.xr, self.z, self.c)
        self.L = self.dev(self.xl, self.z, self.c)
        self.D = self.dev(self.x, self.z, self.o)
        self.U = self.dev(self.x, lax.rem(self.z + 1, 4), self.c)
        self.N = self.dev(self.x, lax.rem(self.z + 3, 4), self.c)
        self.S = ((self.zh * 4 + self.y) * 2 + self.o, self.x * 2 + 1 - self.zl)

    def dev(self, x, z, c):
        return ((lax.div(z, 2) * 4 + self.y) * 2 + c, x * 2 + lax.rem(z, 2))

    def row_dev(self, row):
        return (lax.div(row, 2) * 2 + self.c, self.x * 2 + lax.rem(row, 2))


def greet(devices):
    barrier = pltpu.get_barrier_semaphore()
    for device in devices:
        pl.semaphore_signal(barrier, inc=1, device_id=device, device_id_type=MESH)
    pl.semaphore_wait(barrier, len(devices))


def blk(x, c, width=B, off=0):
    return pl.ds(pl.multiple_of((x * 2 + c) * B + off, 128), width)


class Gather:
    KINDS = 9

    def __init__(self, p, full, rows, ss, rs):
        self.p, self.full, self.rows, self.ss, self.rs = p, full, rows, ss, rs
        x, c, o = p.x, p.c, p.o
        H = 128
        self.sent = [
            (blk(x, c), p.R), (blk(x, c), p.L), (blk(x, c), p.D),
            (blk(p.xl, c, H), p.R), (blk(p.xr, c, H, H), p.L),
            (blk(p.xl, c), p.D), (blk(p.xr, c), p.D),
            (blk(p.xf, c, H), p.D), (blk(p.xf, c, H, H), p.D),
        ]
        self.landed = [
            blk(p.xl, c), blk(p.xr, c), blk(x, o),
            blk(p.xf, c, H), blk(p.xf, c, H, H),
            blk(p.xl, o), blk(p.xr, o),
            blk(p.xf, o, H), blk(p.xf, o, H, H),
        ]

    def out(self, k, t):
        cols, dev = self.sent[k]
        ref = self.full.at[(*self.rows(t), cols)]
        return rc(ref, ref, self.ss.at[k, t], self.rs.at[k, t], dev)

    def got(self, k, t):
        ref = self.full.at[(*self.rows(t), self.landed[k])]
        rc(ref, ref, self.ss.at[k, t], self.rs.at[k, t], self.sent[k][1]).wait_recv()

    def own(self, t):
        for k in (0, 1, 2):
            self.out(k, t).start()

    def relay(self, t):
        self.got(0, t)
        self.out(3, t).start()
        self.out(5, t).start()
        self.got(1, t)
        self.out(4, t).start()
        self.out(6, t).start()

    def far(self, t):
        self.got(3, t)
        self.out(7, t).start()
        self.got(4, t)
        self.out(8, t).start()

    def arrive(self, t):
        for k in (2, 5, 6, 7, 8):
            self.got(k, t)

    def drain(self, t):
        for k in range(9):
            self.out(k, t).wait_send()


class Reduce:
    def __init__(self, p, ch, act, half, w, part, fs, fr, ns, nr, ss, rs):
        self.p, self.ch, self.act, self.half, self.w, self.part = p, ch, act, half, w, part
        self.fs, self.fr, self.ns, self.nr, self.ss, self.rs = fs, fr, ns, nr, ss, rs

    def r(self, t):
        return pl.ds(pl.multiple_of(t * self.ch, self.ch), self.ch)

    def copy(self, k, t):
        p, r = self.p, self.r(t)
        if k == 0:
            src, dst, dev = self.act.at[r, 0 : self.half], self.act.at[r, self.half : 2 * self.half], p.D
        elif k in (1, 2):
            src, dst, dev = self.fs.at[k - 1, r], self.fr.at[k - 1, r], (p.R, p.L)[k - 1]
        else:
            src, dst, dev = self.ns.at[k - 3, r], self.nr.at[k - 3, r], (p.R, p.L)[k - 3]
        return rc(src, dst, self.ss.at[k, t], self.rs.at[k, t], dev)

    def share(self, t):
        self.copy(0, t).start()

    def project(self, t):
        r = self.r(t)
        self.copy(0, t).wait_recv()
        out = jnp.dot(self.act[r, :], self.w[...], preferred_element_type=F32)
        self.fs[0, r] = out[:, 512:640].astype(BF)
        self.fs[1, r] = out[:, 640:768].astype(BF)
        self.copy(1, t).start()
        self.copy(2, t).start()
        self.part[r, 0:512] = out[:, 0:512]
        self.part[r, 512:768] = out[:, 768:1024]

    def near(self, t):
        r = self.r(t)
        self.copy(1, t).wait_recv()
        self.ns[0, r, 0:128] = (self.part[r, 256:384] + self.fr[0, r].astype(F32)).astype(BF)
        self.ns[0, r, 128:256] = self.part[r, 384:512].astype(BF)
        self.copy(3, t).start()
        self.copy(2, t).wait_recv()
        self.ns[1, r, 0:128] = self.part[r, 512:640].astype(BF)
        self.ns[1, r, 128:256] = (self.part[r, 640:768] + self.fr[1, r].astype(F32)).astype(BF)
        self.copy(4, t).start()

    def total(self, t):
        r = self.r(t)
        self.copy(3, t).wait_recv()
        self.copy(4, t).wait_recv()
        return self.part[r, 0:256] + self.nr[0, r].astype(F32) + self.nr[1, r].astype(F32)

    def drain(self, t):
        for k in range(5):
            self.copy(k, t).wait_send()


def normed(values, mod, row):
    v = values.astype(F32)
    v = v - jnp.mean(v, axis=-1, keepdims=True)
    v = v * lax.rsqrt(jnp.mean(v * v, axis=-1, keepdims=True) + 1e-06)
    return (v * (1.0 + mod[row + 1 : row + 2, :]) + mod[row : row + 1, :]).astype(BF)


def each(n, function):
    def body(i, carry):
        function(i)
        return carry

    lax.fori_loop(0, n, body, 0)


class QKV:
    def __init__(self, p, w, mine, theirs, ss, rs, ls):
        self.p, self.w, self.mine, self.theirs, self.ss, self.rs, self.ls = p, w, mine, theirs, ss, rs, ls
        self.half = pl.ds(pl.multiple_of(p.c * 128, 128), 128)

    def locals(self):
        return [
            pltpu.make_async_copy(self.w.at[j, :, self.half], self.mine.at[:, j * 128 : j * 128 + 128], self.ls.at[j])
            for j in range(3)
        ]

    def piece(self, i):
        for d, dev in enumerate((self.p.U, self.p.N)):
            rows = pl.ds(pl.multiple_of(d * 1024 + i * 128, 128), 128)
            for j in range(3):
                rc(
                    self.w.at[j, rows, self.half], self.theirs.at[rows, j * 128 : j * 128 + 128],
                    self.ss.at[d], self.rs.at[d], dev,
                ).start()

    def whole(self, d):
        ref = self.theirs.at[d * 1024 : d * 1024 + 1024, :]
        return rc(ref, ref, self.ss.at[d], self.rs.at[d], (self.p.U, self.p.N)[d])


class Out:
    def __init__(self, p, w, dst, rows, ss, rs, ls):
        self.p, self.w, self.dst, self.rows, self.ss, self.rs, self.ls = p, w, dst, rows, ss, rs, ls

    def src(self, g, j, first, count):
        start = (self.p.c, self.p.o)[g] * self.rows + first
        return self.w.at[pl.ds(pl.multiple_of(start, 128), count), blk(lax.rem(self.p.x + j, 4), self.p.c)]

    def locals(self):
        n = self.rows
        return [
            pltpu.make_async_copy(
                self.src(g, j, 0, n), self.dst.at[2 * g * n : 2 * g * n + n, j * B : j * B + B], self.ls.at[g * 4 + j]
            )
            for g in range(2)
            for j in range(4)
        ]

    def piece(self, i):
        n = self.rows
        per = n // 128
        j, first = lax.div(i, per), lax.rem(i, per) * 128
        for g, dev in enumerate((self.p.U, self.p.N)):
            rows = pl.ds(pl.multiple_of((2 * g + 1) * n + first, 128), 128)
            rc(
                self.src(g, j, first, 128), self.dst.at[rows, pl.ds(pl.multiple_of(j * B, B), B)],
                self.ss.at[g], self.rs.at[g], dev,
            ).start()

    def whole(self, g):
        n = self.rows
        ref = self.dst.at[(2 * g + 1) * n : (2 * g + 2) * n, :]
        return rc(ref, ref, self.ss.at[g], self.rs.at[g], (self.p.U, self.p.N)[g])


class Hidden:
    def __init__(self, p, w, dst, ss, rs, ls):
        self.p, self.w, self.dst, self.ss, self.rs, self.ls = p, w, dst, ss, rs, ls
        self.half = pl.ds(pl.multiple_of(p.c * 512, 512), 512)

    def locals(self):
        return [pltpu.make_async_copy(self.w.at[:, self.half], self.dst.at[:, 0:512], self.ls.at[0])]

    def piece(self, i):
        for d, dev in enumerate((self.p.U, self.p.N)):
            rows = pl.ds(pl.multiple_of(d * 1024 + i * 64, 64), 64)
            rc(
                self.w.at[rows, self.half], self.dst.at[rows, 512:1024], self.ss.at[d], self.rs.at[d], dev
            ).start()

    def whole(self, d):
        ref = self.dst.at[d * 1024 : d * 1024 + 1024, 512:1024]
        return rc(ref, ref, self.ss.at[d], self.rs.at[d], (self.p.U, self.p.N)[d])


def ready(weights):
    for d in range(2):
        weights.whole(d).wait_recv()
    for copy in weights.locals():
        copy.wait()


DMA = pltpu.SemaphoreType.DMA
NC, CH = 8, 128


def rows_of(t):
    return pl.ds(pl.multiple_of(t * CH, CH), CH)


def flat_rows(t):
    return (rows_of(t),)


def lanes(rows):
    return lax.broadcasted_iota(jnp.int32, (rows, 128), 1)


def head_pair(q, k, v, mask):
    lane = lanes(q.shape[0])
    outs = []
    for a in range(2):
        qa = jnp.where((lane < 64) == (a == 0), q, jnp.zeros_like(q))
        s = lax.dot_general(qa, k, (((1,), (1,)), ((), ())), preferred_element_type=F32)
        if mask is not None:
            s = jnp.where(mask, s, -1e30)
        e = jnp.exp(s - jnp.max(s, axis=-1, keepdims=True)).astype(BF)
        o = jnp.dot(e, v, preferred_element_type=F32)
        outs.append(o[:, 0:128] / o[:, 128:256])
    return jnp.where(lane < 64, outs[0], outs[1]).astype(BF)


PROJECT, NEAR, FINISH = 1, 3, 5
ENTER, RELAY, FAR, COMPUTE = 8, 10, 12, 13
PROJECT2, NEAR2, FINISH2 = 14, 16, 18
RELAY2, FAR2, COMPUTE2 = 20, 22, 23
PROJECT3, NEAR3, FINISH3 = 24, 26, 28
PLAN = ((1, 4, 1), (5, 4, 1), (9, 4, 2), (13, 10, 2))


def block(
    latent, mod, sw, so, tw, to, hw, ow, out,
    qkv, full0, nrm, mine0, theirs0, g0, h0, zs, zr, zl_, ls0, ss0, sr0,
    vx, ws, one, full1, mine, theirs, wt, full2, w1, w2, res, part,
    a1, fs1, fr1, ns1, nr1, a2, fs2, fr2, ns2, nr2, a3, fs3, fr3, ns3, nr3,
    s1, v1, s2, v2, s3, v3, g1, h1, g2, h2,
    ps, pr, qs, qr, us, ur, hs, hr, os, orr, pl_, ql, ul, hl, ol, xs, xr, ls, ss, sr,
):
    p = Place()
    greet([p.L, p.R, p.D, p.S] + [p.row_dev(lax.rem(p.row + k, 16)) for k in range(1, 16)])
    here = blk(p.x, p.c)
    wsq = QKV(p, sw, mine0, theirs0, zs, zr, zl_)
    gat0 = Gather(p, full0, flat_rows, g0, h0)
    wso = Out(p, so, ws, 128, ps, pr, pl_)
    wtq = QKV(p, tw, mine, theirs, qs, qr, ql)
    wto = Out(p, to, wt, 128, us, ur, ul)
    whi = Hidden(p, hw, w1, hs, hr, hl)
    wou = Out(p, ow, w2, 512, os, orr, ol)
    r1 = Reduce(p, CH, a1, 256, ws, part, fs1, fr1, ns1, nr1, s1, v1)
    r2 = Reduce(p, CH, a2, 256, wt, part, fs2, fr2, ns2, nr2, s2, v2)
    r3 = Reduce(p, CH, a3, 1024, w2, part, fs3, fr3, ns3, nr3, s3, v3)
    gat1 = Gather(p, full1, flat_rows, g1, h1)
    gat2 = Gather(p, full2, flat_rows, g2, h2)

    def eight(t, row):
        return pl.ds(pl.multiple_of(t * CH + row * 8, 8), 8)

    def strip(t, row):
        return pl.ds(pl.multiple_of(row * 64 + t * 8, 8), 8)

    def keep(t):
        each(16, lambda k: pltpu.make_async_copy(latent.at[strip(t, k), :], full0.at[eight(t, k), here], ls0.at[t]).start())

    def kept(t):
        r = rows_of(t)
        return pltpu.make_async_copy(latent.at[r, :], full0.at[r, here], ls0.at[t])

    def swap(t):
        there = blk(p.x, p.o)
        each(
            16,
            lambda k: rc(
                latent.at[strip(t, k), :], full0.at[eight(t, k), there], ss0.at[t], sr0.at[t], p.S
            ).start(),
        )

    def swapped(t):
        r = rows_of(t)
        return rc(latent.at[r, :], full0.at[r, here], ss0.at[t], sr0.at[t], p.S)

    @pl.when(p.c == p.zl)
    def _():
        each(NC, keep)

    @pl.when(p.c != p.zl)
    def _():
        each(NC, swap)

    for copy in wsq.locals():
        copy.start()
    each(NC, wsq.piece)
    each(4, wso.piece)
    for weights in (wso, wtq, wto, whi, wou):
        for copy in weights.locals():
            copy.start()

    def first(t):
        @pl.when(p.c == p.zl)
        def _():
            kept(t).wait()

        @pl.when(p.c != p.zl)
        def _():
            swapped(t).wait_recv()

        gat0.own(t)

    def spatial(t):
        @pl.when(t == 0)
        def _():
            for copy in wsq.locals():
                copy.wait()

        gat0.arrive(t)
        r = rows_of(t)
        nrm[r, :] = normed(full0[r, :], mod, 0)
        qkv[r, 0:384] = jnp.dot(nrm[r, :], mine0[...], preferred_element_type=F32).astype(BF)

    def spatial_rest(t):
        @pl.when(t == 0)
        def _():
            for d in range(2):
                wsq.whole(d).wait_recv()

        r = rows_of(t)
        qkv[r, 384:768] = jnp.dot(nrm[r, :], theirs0[...], preferred_element_type=F32).astype(BF)

    def steps(total, *entries):
        def body(i, carry):
            for start, count, function in entries:

                @pl.when((i >= start) & (i < start + count))
                def _(t=i - start, function=function):
                    function(t)

            return carry

        lax.fori_loop(0, total, body, 0)

    steps(
        NC + 10,
        (0, NC, first), (2, NC, gat0.relay), (4, NC, gat0.far), (6, 8, wtq.piece), (6, NC, spatial), (10, NC, spatial_rest),
    )
    for pair in range(2):
        vx[pair, :, 0:128] = qkv[:, pair * 384 + 256 : pair * 384 + 384]
        vx[pair, :, 128:256] = jnp.ones((T, 128), BF)

    def heads(t):
        r = rows_of(t)
        for pair in range(2):
            base = pair * 384
            q = qkv[r, base : base + 128] * jnp.array(0.125, BF)
            a1[r, pair * 128 : pair * 128 + 128] = head_pair(q, qkv[:, base + 128 : base + 256], vx[pair], None)
        r1.share(t)

    def project1(t):
        @pl.when(t == 0)
        def _():
            ready(wso)

        r1.project(t)

    def cross(k, t):
        row = lax.rem(p.row + k, 16)
        return rc(one.at[eight(t, row), :], full1.at[eight(t, p.row), here], xs.at[k, t], xr.at[p.row, t], p.row_dev(row))

    def stay(t):
        return pltpu.make_async_copy(one.at[eight(t, p.row), :], full1.at[eight(t, p.row), here], xr.at[p.row, t])

    def finish1(t):
        r = rows_of(t)
        gate = mod[2:3, here]
        one[r, :] = (full0[r, here].astype(F32) + gate * r1.total(t)).astype(BF)
        each(15, lambda k: cross(k + 1, t).start())
        stay(t).start()

    def enter1(t):
        def arrived(k):
            row = lax.rem(p.row + k, 16)
            rc(
                one.at[eight(t, row), :], full1.at[eight(t, row), here], xs.at[k, t], xr.at[row, t], p.row_dev(row)
            ).wait_recv()

        each(15, lambda k: arrived(k + 1))
        stay(t).wait()
        gat1.own(t)

    i = lax.broadcasted_iota(jnp.int32, (CH, CH), 0)
    j = lax.broadcasted_iota(jnp.int32, (CH, CH), 1)
    same = lax.rem(i, 8) == lax.rem(j, 8)

    def temporal(t):
        @pl.when(t == 0)
        def _():
            ready(wtq)

        gat1.arrive(t)
        r = rows_of(t)
        n = normed(full1[r, :], mod, 3)
        for pair, w in enumerate((mine, theirs)):
            y = jnp.dot(n, w[...], preferred_element_type=F32).astype(BF)
            v = jnp.concatenate([y[:, 256:384], jnp.ones((CH, 128), BF)], axis=1)
            a2[r, pair * 128 : pair * 128 + 128] = head_pair(
                y[:, 0:128] * jnp.array(0.125, BF), y[:, 128:256], v, same
            )
        r2.share(t)

    def project2(t):
        @pl.when(t == 0)
        def _():
            ready(wto)

        r2.project(t)

    def finish2(t):
        r = rows_of(t)
        gate = mod[5:6, here]
        full2[r, here] = (full1[r, here].astype(F32) + gate * r2.total(t)).astype(BF)
        gat2.own(t)

    def hidden(t):
        @pl.when(t == 0)
        def _():
            ready(whi)

        gat2.arrive(t)
        r = rows_of(t)
        h = jnp.dot(normed(full2[r, :], mod, 6), w1[...], preferred_element_type=F32)
        h = 0.5 * h * (1.0 + jnp.tanh(0.7978845608028654 * (h + 0.044715 * (h * h * h))))
        a3[r, 0:1024] = h.astype(BF)
        r3.share(t)

    def project3(t):
        @pl.when(t == 0)
        def _():
            ready(wou)

        r3.project(t)

    def put(t):
        each(16, lambda k: pltpu.make_async_copy(res.at[eight(t, k), :], out.at[strip(t, k), :], ls.at[t]).start())

    def putted(t):
        r = rows_of(t)
        return pltpu.make_async_copy(res.at[r, :], out.at[r, :], ls.at[t])

    def back(t):
        each(16, lambda k: rc(res.at[eight(t, k), :], out.at[strip(t, k), :], ss.at[t], sr.at[t], p.S).start())

    def backed(t):
        r = rows_of(t)
        return rc(res.at[r, :], out.at[r, :], ss.at[t], sr.at[t], p.S)

    def finish3(t):
        r = rows_of(t)
        gate = mod[8:9, here]
        res[r, :] = (full2[r, here].astype(F32) + gate * r3.total(t)).astype(BF)

        @pl.when(p.c == p.zl)
        def _():
            put(t)

        @pl.when(p.c != p.zl)
        def _():
            back(t)

    def pace(plan):
        order = [(wto, n) for n in range(4)] + [(whi, n) for n in range(16)] + [(wou, n) for n in range(16)]
        runs = []
        for start, count, rate in plan:
            for step in range(start, start + count):
                for weights, n in order[:rate]:
                    last = runs[-1] if runs else None
                    if last and last[0] is weights and last[2] == rate and (n - last[3]) // rate == step - last[1]:
                        last[4] = n + 1
                    else:
                        runs.append([weights, step, rate, n, n + 1])
                order = order[rate:]
        assert not order

        def entry(weights, step, rate, low, high):
            def run(i):
                for k in range(rate):
                    n = low + rate * i + k
                    if (high - low) % rate == 0:
                        weights.piece(n)
                    else:

                        @pl.when(n < high)
                        def _(n=n):
                            weights.piece(n)

            return step, -(-(high - low) // rate), run

        return [entry(*run) for run in runs]

    steps(
        NC + FINISH3,
        (NEAR, NC, r1.near), (NEAR2, NC, r2.near), (NEAR3, NC, r3.near),
        (FINISH, NC, finish1), (RELAY, NC, gat1.relay), (FAR, NC, gat1.far),
        (FINISH2, NC, finish2), (RELAY2, NC, gat2.relay), (FAR2, NC, gat2.far), (FINISH3, NC, finish3),
        (PROJECT, NC, project1), (PROJECT2, NC, project2), (PROJECT3, NC, project3), (ENTER, NC, enter1),
        *pace(PLAN), (0, NC, heads), (COMPUTE, NC, temporal), (COMPUTE2, NC, hidden),
    )

    def drain(t):
        for stage in (r1, r2, r3, gat0, gat1, gat2):
            stage.drain(t)
        each(15, lambda k: cross(k + 1, t).wait_send())

    each(NC, drain)
    for weights in (wsq, wso, wtq, wto, whi, wou):
        for d in range(2):
            weights.whole(d).wait_send()

    @pl.when(p.c != p.zl)
    def _():
        each(NC, lambda t: swapped(t).wait_send())

    @pl.when(p.c == p.zl)
    def _():
        each(NC, lambda t: putted(t).wait())

    @pl.when(p.c != p.zl)
    def _():
        each(NC, lambda t: backed(t).wait())


def call(kernel, name, ident, ins, outs, scratch, limit, cost):
    return pl.pallas_call(
        kernel,
        name=name,
        out_shape=[jax.ShapeDtypeStruct(shape, BF) for shape, _ in outs],
        in_specs=ins,
        out_specs=[spec for _, spec in outs],
        scratch_shapes=scratch,
        compiler_params=pltpu.CompilerParams(
            collective_id=ident, has_side_effects=True, vmem_limit_bytes=limit << 20
        ),
        cost_estimate=pl.CostEstimate(flops=cost, bytes_accessed=1 << 24, transcendentals=0),
    )


def input_scratch():
    return [
        VM((T, 768), BF), VM((T, D), BF), VM((T, D), BF), VM((D, 384), BF), VM((D, 384), BF),
        DMA((9, NC)), DMA((9, NC)), DMA((2,)), DMA((2,)), DMA((3,)), DMA((NC,)), DMA((NC,)), DMA((NC,)),
    ]


def tail_scratch():
    def reduce(width):
        return [VM((T, width), BF), VM((2, T, 128), BF), VM((2, T, 128), BF), VM((2, T, B), BF), VM((2, T, B), BF)]

    pair = [DMA((2,)), DMA((2,))]
    return (
        [VM((2, T, B), BF), VM((512, 1024), BF), VM((T, B), BF), VM((T, D), BF), VM((D, 384), BF), VM((D, 384), BF)]
        + [VM((512, 1024), BF), VM((T, D), BF), VM((D, 1024), BF), VM((D, 1024), BF), VM((T, B), BF), VM((T, 768), F32)]
        + reduce(512) + reduce(512) + reduce(2048)
        + [DMA((5, NC))] * 6 + [DMA((9, NC))] * 4
        + pair * 5 + [DMA((8,)), DMA((3,)), DMA((8,)), DMA((1,)), DMA((8,))]
        + [DMA((16, NC)), DMA((16, NC)), DMA((NC,)), DMA((NC,)), DMA((NC,))]
    )


def per_device(latent, mod, *weights):
    (out,) = call(
        block, "block", 0, [ANY, INV] + [ANY] * 6, [((T, B), ANY)], input_scratch() + tail_scratch(), 63, 4 * 10**10
    )(latent.reshape(T, B), mod, *weights)
    return out.reshape(16, 64, B)


def solution(mesh):
    in_specs = (
        P("seq", None, "head"), P(), P(None, None, "head"), P("head", None),
        P(None, None, "head"), P("head", None), P(None, "head"), P("head", None),
    )
    return jax.shard_map(
        per_device, mesh=mesh, in_specs=in_specs, out_specs=P(None, "seq", "head"), check_vma=False
    )
```

```python
import functools

import jax
import jax.numpy as jnp
from jax import lax
from jax.experimental import pallas as pl
from jax.experimental.pallas import tpu as pltpu
from jax.sharding import PartitionSpec as P

MESH = pl.DeviceIdType.MESH
BF = jnp.bfloat16
F32 = jnp.float32
T = 1024
D = 2048
B = 256
VM = pltpu.VMEM
ANY = pl.BlockSpec(memory_space=pltpu.MemorySpace.HBM)
INV = pl.BlockSpec(memory_space=pltpu.VMEM)


def rc(src, dst, ss, rs, dev):
    return pltpu.make_async_remote_copy(
        src_ref=src, dst_ref=dst, send_sem=ss, recv_sem=rs, device_id=dev, device_id_type=MESH
    )


class Place:
    def __init__(self):
        s, h = lax.axis_index("seq"), lax.axis_index("head")
        self.c, self.y, self.zh = lax.rem(s, 2), lax.rem(lax.div(s, 2), 4), lax.div(s, 8)
        self.x, self.zl = lax.div(h, 2), lax.rem(h, 2)
        self.z = self.zh * 2 + self.zl
        self.o = 1 - self.c
        self.row = (self.zh * 4 + self.y) * 2 + self.zl
        self.xr, self.xl, self.xf = [lax.rem(self.x + k, 4) for k in (1, 3, 2)]
        self.R = self.dev(self.xr, self.z, self.c)
        self.L = self.dev(self.xl, self.z, self.c)
        self.D = self.dev(self.x, self.z, self.o)
        self.U = self.dev(self.x, lax.rem(self.z + 1, 4), self.c)
        self.N = self.dev(self.x, lax.rem(self.z + 3, 4), self.c)
        self.S = ((self.zh * 4 + self.y) * 2 + self.o, self.x * 2 + 1 - self.zl)

    def dev(self, x, z, c):
        return ((lax.div(z, 2) * 4 + self.y) * 2 + c, x * 2 + lax.rem(z, 2))

    def row_dev(self, row):
        return (lax.div(row, 2) * 2 + self.c, self.x * 2 + lax.rem(row, 2))


def greet(devices):
    barrier = pltpu.get_barrier_semaphore()
    for device in devices:
        pl.semaphore_signal(barrier, inc=1, device_id=device, device_id_type=MESH)
    pl.semaphore_wait(barrier, len(devices))


def blk(x, c, width=B, off=0):
    return pl.ds(pl.multiple_of((x * 2 + c) * B + off, 128), width)


class Gather:
    KINDS = 9

    def __init__(self, p, full, rows, ss, rs):
        self.p, self.full, self.rows, self.ss, self.rs = p, full, rows, ss, rs
        x, c, o = p.x, p.c, p.o
        H = 128
        self.sent = [
            (blk(x, c), p.R), (blk(x, c), p.L), (blk(x, c), p.D),
            (blk(p.xl, c, H), p.R), (blk(p.xr, c, H, H), p.L),
            (blk(p.xl, c), p.D), (blk(p.xr, c), p.D),
            (blk(p.xf, c, H), p.D), (blk(p.xf, c, H, H), p.D),
        ]
        self.landed = [
            blk(p.xl, c), blk(p.xr, c), blk(x, o),
            blk(p.xf, c, H), blk(p.xf, c, H, H),
            blk(p.xl, o), blk(p.xr, o),
            blk(p.xf, o, H), blk(p.xf, o, H, H),
        ]

    def out(self, k, t):
        cols, dev = self.sent[k]
        ref = self.full.at[(*self.rows(t), cols)]
        return rc(ref, ref, self.ss.at[k, t], self.rs.at[k, t], dev)

    def got(self, k, t):
        ref = self.full.at[(*self.rows(t), self.landed[k])]
        rc(ref, ref, self.ss.at[k, t], self.rs.at[k, t], self.sent[k][1]).wait_recv()

    def own(self, t):
        for k in (0, 1, 2):
            self.out(k, t).start()

    def relay(self, t):
        self.got(0, t)
        self.out(3, t).start()
        self.out(5, t).start()
        self.got(1, t)
        self.out(4, t).start()
        self.out(6, t).start()

    def far(self, t):
        self.got(3, t)
        self.out(7, t).start()
        self.got(4, t)
        self.out(8, t).start()

    def arrive(self, t):
        for k in (2, 5, 6, 7, 8):
            self.got(k, t)

    def drain(self, t):
        for k in range(9):
            self.out(k, t).wait_send()


class Reduce:
    def __init__(self, p, ch, act, half, w, part, fs, fr, ns, nr, ss, rs):
        self.p, self.ch, self.act, self.half, self.w, self.part = p, ch, act, half, w, part
        self.fs, self.fr, self.ns, self.nr, self.ss, self.rs = fs, fr, ns, nr, ss, rs

    def r(self, t):
        return pl.ds(pl.multiple_of(t * self.ch, self.ch), self.ch)

    def copy(self, k, t):
        p, r = self.p, self.r(t)
        if k == 0:
            src, dst, dev = self.act.at[r, 0 : self.half], self.act.at[r, self.half : 2 * self.half], p.D
        elif k in (1, 2):
            src, dst, dev = self.fs.at[k - 1, r], self.fr.at[k - 1, r], (p.R, p.L)[k - 1]
        else:
            src, dst, dev = self.ns.at[k - 3, r], self.nr.at[k - 3, r], (p.R, p.L)[k - 3]
        return rc(src, dst, self.ss.at[k, t], self.rs.at[k, t], dev)

    def share(self, t):
        self.copy(0, t).start()

    def project(self, t):
        r = self.r(t)
        self.copy(0, t).wait_recv()
        out = jnp.dot(self.act[r, :], self.w[...], preferred_element_type=F32)
        self.fs[0, r] = out[:, 512:640].astype(BF)
        self.fs[1, r] = out[:, 640:768].astype(BF)
        self.copy(1, t).start()
        self.copy(2, t).start()
        self.part[r, 0:512] = out[:, 0:512]
        self.part[r, 512:768] = out[:, 768:1024]

    def near(self, t):
        r = self.r(t)
        self.copy(1, t).wait_recv()
        self.ns[0, r, 0:128] = (self.part[r, 256:384] + self.fr[0, r].astype(F32)).astype(BF)
        self.ns[0, r, 128:256] = self.part[r, 384:512].astype(BF)
        self.copy(3, t).start()
        self.copy(2, t).wait_recv()
        self.ns[1, r, 0:128] = self.part[r, 512:640].astype(BF)
        self.ns[1, r, 128:256] = (self.part[r, 640:768] + self.fr[1, r].astype(F32)).astype(BF)
        self.copy(4, t).start()

    def total(self, t):
        r = self.r(t)
        self.copy(3, t).wait_recv()
        self.copy(4, t).wait_recv()
        return self.part[r, 0:256] + self.nr[0, r].astype(F32) + self.nr[1, r].astype(F32)

    def drain(self, t):
        for k in range(5):
            self.copy(k, t).wait_send()


def normed(values, mod, row):
    v = values.astype(F32)
    v = v - jnp.mean(v, axis=-1, keepdims=True)
    v = v * lax.rsqrt(jnp.mean(v * v, axis=-1, keepdims=True) + 1e-06)
    return (v * (1.0 + mod[row + 1 : row + 2, :]) + mod[row : row + 1, :]).astype(BF)


def each(n, function):
    def body(i, carry):
        function(i)
        return carry

    lax.fori_loop(0, n, body, 0)


class QKV:
    def __init__(self, p, w, mine, theirs, ss, rs, ls):
        self.p, self.w, self.mine, self.theirs, self.ss, self.rs, self.ls = p, w, mine, theirs, ss, rs, ls
        self.half = pl.ds(pl.multiple_of(p.c * 128, 128), 128)

    def locals(self):
        return [
            pltpu.make_async_copy(self.w.at[j, :, self.half], self.mine.at[:, j * 128 : j * 128 + 128], self.ls.at[j])
            for j in range(3)
        ]

    def piece(self, i):
        for d, dev in enumerate((self.p.U, self.p.N)):
            rows = pl.ds(pl.multiple_of(d * 1024 + i * 128, 128), 128)
            for j in range(3):
                rc(
                    self.w.at[j, rows, self.half], self.theirs.at[rows, j * 128 : j * 128 + 128],
                    self.ss.at[d], self.rs.at[d], dev,
                ).start()

    def whole(self, d):
        ref = self.theirs.at[d * 1024 : d * 1024 + 1024, :]
        return rc(ref, ref, self.ss.at[d], self.rs.at[d], (self.p.U, self.p.N)[d])


class Out:
    def __init__(self, p, w, dst, rows, ss, rs, ls):
        self.p, self.w, self.dst, self.rows, self.ss, self.rs, self.ls = p, w, dst, rows, ss, rs, ls

    def src(self, g, j, first, count):
        start = (self.p.c, self.p.o)[g] * self.rows + first
        return self.w.at[pl.ds(pl.multiple_of(start, 128), count), blk(lax.rem(self.p.x + j, 4), self.p.c)]

    def locals(self):
        n = self.rows
        return [
            pltpu.make_async_copy(
                self.src(g, j, 0, n), self.dst.at[2 * g * n : 2 * g * n + n, j * B : j * B + B], self.ls.at[g * 4 + j]
            )
            for g in range(2)
            for j in range(4)
        ]

    def piece(self, i):
        n = self.rows
        per = n // 128
        j, first = lax.div(i, per), lax.rem(i, per) * 128
        for g, dev in enumerate((self.p.U, self.p.N)):
            rows = pl.ds(pl.multiple_of((2 * g + 1) * n + first, 128), 128)
            rc(
                self.src(g, j, first, 128), self.dst.at[rows, pl.ds(pl.multiple_of(j * B, B), B)],
                self.ss.at[g], self.rs.at[g], dev,
            ).start()

    def whole(self, g):
        n = self.rows
        ref = self.dst.at[(2 * g + 1) * n : (2 * g + 2) * n, :]
        return rc(ref, ref, self.ss.at[g], self.rs.at[g], (self.p.U, self.p.N)[g])


class Hidden:
    def __init__(self, p, w, dst, ss, rs, ls):
        self.p, self.w, self.dst, self.ss, self.rs, self.ls = p, w, dst, ss, rs, ls
        self.half = pl.ds(pl.multiple_of(p.c * 512, 512), 512)

    def locals(self):
        return [pltpu.make_async_copy(self.w.at[:, self.half], self.dst.at[:, 0:512], self.ls.at[0])]

    def piece(self, i):
        for d, dev in enumerate((self.p.U, self.p.N)):
            rows = pl.ds(pl.multiple_of(d * 1024 + i * 64, 64), 64)
            rc(
                self.w.at[rows, self.half], self.dst.at[rows, 512:1024], self.ss.at[d], self.rs.at[d], dev
            ).start()

    def whole(self, d):
        ref = self.dst.at[d * 1024 : d * 1024 + 1024, 512:1024]
        return rc(ref, ref, self.ss.at[d], self.rs.at[d], (self.p.U, self.p.N)[d])


def ready(weights):
    for d in range(2):
        weights.whole(d).wait_recv()
    for copy in weights.locals():
        copy.wait()


DMA = pltpu.SemaphoreType.DMA
NC, CH = 8, 128


def rows_of(t):
    return pl.ds(pl.multiple_of(t * CH, CH), CH)


def flat_rows(t):
    return (rows_of(t),)


def lanes(rows):
    return lax.broadcasted_iota(jnp.int32, (rows, 128), 1)


def head_pair(q, k, v, mask):
    lane = lanes(q.shape[0])
    outs = []
    for a in range(2):
        qa = jnp.where((lane < 64) == (a == 0), q, jnp.zeros_like(q))
        s = lax.dot_general(qa, k, (((1,), (1,)), ((), ())), preferred_element_type=F32)
        if mask is not None:
            s = jnp.where(mask, s, -1e30)
        e = jnp.exp(s - jnp.max(s, axis=-1, keepdims=True)).astype(BF)
        o = jnp.dot(e, v, preferred_element_type=F32)
        outs.append(o[:, 0:128] / o[:, 128:256])
    return jnp.where(lane < 64, outs[0], outs[1]).astype(BF)


PROJECT, NEAR, FINISH = 1, 3, 5
ENTER, RELAY, FAR, COMPUTE = 8, 10, 12, 13
PROJECT2, NEAR2, FINISH2 = 14, 16, 18
RELAY2, FAR2, COMPUTE2 = 20, 22, 23
PROJECT3, NEAR3, FINISH3 = 24, 26, 28
PLAN = ((0, 10, 1), (10, 13, 2))


def block(
    latent, mod, sw, so, tw, to, hw, ow, out,
    qkv, full0, nrm, mine0, theirs0, g0, h0, zs, zr, zl_, ls0, ss0, sr0,
    vx, ws, one, full1, mine, theirs, wt, full2, w1, w2, res, part,
    a1, fs1, fr1, ns1, nr1, a2, fs2, fr2, ns2, nr2, a3, fs3, fr3, ns3, nr3,
    s1, v1, s2, v2, s3, v3, g1, h1, g2, h2,
    ps, pr, qs, qr, us, ur, hs, hr, os, orr, pl_, ql, ul, hl, ol, xs, xr, ls, ss, sr,
):
    p = Place()
    greet([p.L, p.R, p.D, p.S] + [p.row_dev(lax.rem(p.row + k, 16)) for k in range(1, 16)])
    here = blk(p.x, p.c)
    wsq = QKV(p, sw, mine0, theirs0, zs, zr, zl_)
    gat0 = Gather(p, full0, flat_rows, g0, h0)
    wso = Out(p, so, ws, 128, ps, pr, pl_)
    wtq = QKV(p, tw, mine, theirs, qs, qr, ql)
    wto = Out(p, to, wt, 128, us, ur, ul)
    whi = Hidden(p, hw, w1, hs, hr, hl)
    wou = Out(p, ow, w2, 512, os, orr, ol)
    r1 = Reduce(p, CH, a1, 256, ws, part, fs1, fr1, ns1, nr1, s1, v1)
    r2 = Reduce(p, CH, a2, 256, wt, part, fs2, fr2, ns2, nr2, s2, v2)
    r3 = Reduce(p, CH, a3, 1024, w2, part, fs3, fr3, ns3, nr3, s3, v3)
    gat1 = Gather(p, full1, flat_rows, g1, h1)
    gat2 = Gather(p, full2, flat_rows, g2, h2)

    def eight(t, row):
        return pl.ds(pl.multiple_of(t * CH + row * 8, 8), 8)

    def strip(t, row):
        return pl.ds(pl.multiple_of(row * 64 + t * 8, 8), 8)

    def keep(t):
        each(16, lambda k: pltpu.make_async_copy(latent.at[strip(t, k), :], full0.at[eight(t, k), here], ls0.at[t]).start())

    def kept(t):
        r = rows_of(t)
        return pltpu.make_async_copy(latent.at[r, :], full0.at[r, here], ls0.at[t])

    def swap(t):
        there = blk(p.x, p.o)
        each(
            16,
            lambda k: rc(
                latent.at[strip(t, k), :], full0.at[eight(t, k), there], ss0.at[t], sr0.at[t], p.S
            ).start(),
        )

    def swapped(t):
        r = rows_of(t)
        return rc(latent.at[r, :], full0.at[r, here], ss0.at[t], sr0.at[t], p.S)

    @pl.when(p.c == p.zl)
    def _():
        each(NC, keep)

    @pl.when(p.c != p.zl)
    def _():
        each(NC, swap)

    for copy in wsq.locals():
        copy.start()
    each(NC, wsq.piece)
    each(4, wso.piece)
    for weights in (wso, wtq, wto, whi, wou):
        for copy in weights.locals():
            copy.start()

    def first(t):
        @pl.when(p.c == p.zl)
        def _():
            kept(t).wait()

        @pl.when(p.c != p.zl)
        def _():
            swapped(t).wait_recv()

        gat0.own(t)

    def spatial(t):
        @pl.when(t == 0)
        def _():
            for copy in wsq.locals():
                copy.wait()

        gat0.arrive(t)
        r = rows_of(t)
        nrm[r, :] = normed(full0[r, :], mod, 0)
        qkv[r, 0:384] = jnp.dot(nrm[r, :], mine0[...], preferred_element_type=F32).astype(BF)

    def spatial_rest(t):
        @pl.when(t == 0)
        def _():
            for d in range(2):
                wsq.whole(d).wait_recv()

        r = rows_of(t)
        qkv[r, 384:768] = jnp.dot(nrm[r, :], theirs0[...], preferred_element_type=F32).astype(BF)

    def steps(total, *entries):
        def body(i, carry):
            for start, count, function in entries:

                @pl.when((i >= start) & (i < start + count))
                def _(t=i - start, function=function):
                    function(t)

            return carry

        lax.fori_loop(0, total, body, 0)

    steps(
        NC + 9,
        (0, NC, first), (2, NC, gat0.relay), (4, NC, gat0.far), (6, 8, wtq.piece), (5, NC, spatial), (9, NC, spatial_rest),
    )
    for pair in range(2):
        vx[pair, :, 0:128] = qkv[:, pair * 384 + 256 : pair * 384 + 384]
        vx[pair, :, 128:256] = jnp.ones((T, 128), BF)

    def heads(t):
        r = rows_of(t)
        for pair in range(2):
            base = pair * 384
            q = qkv[r, base : base + 128] * jnp.array(0.125, BF)
            a1[r, pair * 128 : pair * 128 + 128] = head_pair(q, qkv[:, base + 128 : base + 256], vx[pair], None)
        r1.share(t)

    def project1(t):
        @pl.when(t == 0)
        def _():
            ready(wso)

        r1.project(t)

    def cross(k, t):
        row = lax.rem(p.row + k, 16)
        return rc(one.at[eight(t, row), :], full1.at[eight(t, p.row), here], xs.at[k, t], xr.at[p.row, t], p.row_dev(row))

    def stay(t):
        return pltpu.make_async_copy(one.at[eight(t, p.row), :], full1.at[eight(t, p.row), here], xr.at[p.row, t])

    def finish1(t):
        r = rows_of(t)
        gate = mod[2:3, here]
        one[r, :] = (full0[r, here].astype(F32) + gate * r1.total(t)).astype(BF)
        each(15, lambda k: cross(k + 1, t).start())
        stay(t).start()

    def enter1(t):
        def arrived(k):
            row = lax.rem(p.row + k, 16)
            rc(
                one.at[eight(t, row), :], full1.at[eight(t, row), here], xs.at[k, t], xr.at[row, t], p.row_dev(row)
            ).wait_recv()

        each(15, lambda k: arrived(k + 1))
        stay(t).wait()
        gat1.own(t)

    i = lax.broadcasted_iota(jnp.int32, (CH, CH), 0)
    j = lax.broadcasted_iota(jnp.int32, (CH, CH), 1)
    same = lax.rem(i, 8) == lax.rem(j, 8)

    def temporal(t):
        @pl.when(t == 0)
        def _():
            ready(wtq)

        gat1.arrive(t)
        r = rows_of(t)
        n = normed(full1[r, :], mod, 3)
        for pair, w in enumerate((mine, theirs)):
            y = jnp.dot(n, w[...], preferred_element_type=F32).astype(BF)
            v = jnp.concatenate([y[:, 256:384], jnp.ones((CH, 128), BF)], axis=1)
            a2[r, pair * 128 : pair * 128 + 128] = head_pair(
                y[:, 0:128] * jnp.array(0.125, BF), y[:, 128:256], v, same
            )
        r2.share(t)

    def project2(t):
        @pl.when(t == 0)
        def _():
            ready(wto)

        r2.project(t)

    def finish2(t):
        r = rows_of(t)
        gate = mod[5:6, here]
        full2[r, here] = (full1[r, here].astype(F32) + gate * r2.total(t)).astype(BF)
        gat2.own(t)

    def hidden(t):
        @pl.when(t == 0)
        def _():
            ready(whi)

        gat2.arrive(t)
        r = rows_of(t)
        h = jnp.dot(normed(full2[r, :], mod, 6), w1[...], preferred_element_type=F32)
        h = 0.5 * h * (1.0 + jnp.tanh(0.7978845608028654 * (h + 0.044715 * (h * h * h))))
        a3[r, 0:1024] = h.astype(BF)
        r3.share(t)

    def project3(t):
        @pl.when(t == 0)
        def _():
            ready(wou)

        r3.project(t)

    def put(t):
        each(16, lambda k: pltpu.make_async_copy(res.at[eight(t, k), :], out.at[strip(t, k), :], ls.at[t]).start())

    def putted(t):
        r = rows_of(t)
        return pltpu.make_async_copy(res.at[r, :], out.at[r, :], ls.at[t])

    def back(t):
        each(16, lambda k: rc(res.at[eight(t, k), :], out.at[strip(t, k), :], ss.at[t], sr.at[t], p.S).start())

    def backed(t):
        r = rows_of(t)
        return rc(res.at[r, :], out.at[r, :], ss.at[t], sr.at[t], p.S)

    def finish3(t):
        r = rows_of(t)
        gate = mod[8:9, here]
        res[r, :] = (full2[r, here].astype(F32) + gate * r3.total(t)).astype(BF)

        @pl.when(p.c == p.zl)
        def _():
            put(t)

        @pl.when(p.c != p.zl)
        def _():
            back(t)

    def pace(plan):
        order = [(wto, n) for n in range(4)] + [(whi, n) for n in range(16)] + [(wou, n) for n in range(16)]
        runs = []
        for start, count, rate in plan:
            for step in range(start, start + count):
                for weights, n in order[:rate]:
                    last = runs[-1] if runs else None
                    if last and last[0] is weights and last[2] == rate and (n - last[3]) // rate == step - last[1]:
                        last[4] = n + 1
                    else:
                        runs.append([weights, step, rate, n, n + 1])
                order = order[rate:]
        assert not order

        def entry(weights, step, rate, low, high):
            def run(i):
                for k in range(rate):
                    n = low + rate * i + k
                    if (high - low) % rate == 0:
                        weights.piece(n)
                    else:

                        @pl.when(n < high)
                        def _(n=n):
                            weights.piece(n)

            return step, -(-(high - low) // rate), run

        return [entry(*run) for run in runs]

    steps(
        NC + FINISH3,
        (NEAR, NC, r1.near), (NEAR2, NC, r2.near), (NEAR3, NC, r3.near),
        (FINISH, NC, finish1), (RELAY, NC, gat1.relay), (FAR, NC, gat1.far),
        (FINISH2, NC, finish2), (RELAY2, NC, gat2.relay), (FAR2, NC, gat2.far), (FINISH3, NC, finish3),
        (PROJECT, NC, project1), (PROJECT2, NC, project2), (PROJECT3, NC, project3), (ENTER, NC, enter1),
        *pace(PLAN), (0, NC, heads), (COMPUTE, NC, temporal), (COMPUTE2, NC, hidden),
    )

    def drain(t):
        for stage in (r1, r2, r3, gat0, gat1, gat2):
            stage.drain(t)
        each(15, lambda k: cross(k + 1, t).wait_send())

    each(NC, drain)
    for weights in (wsq, wso, wtq, wto, whi, wou):
        for d in range(2):
            weights.whole(d).wait_send()

    @pl.when(p.c != p.zl)
    def _():
        each(NC, lambda t: swapped(t).wait_send())

    @pl.when(p.c == p.zl)
    def _():
        each(NC, lambda t: putted(t).wait())

    @pl.when(p.c != p.zl)
    def _():
        each(NC, lambda t: backed(t).wait())


def call(kernel, name, ident, ins, outs, scratch, limit, cost):
    return pl.pallas_call(
        kernel,
        name=name,
        out_shape=[jax.ShapeDtypeStruct(shape, BF) for shape, _ in outs],
        in_specs=ins,
        out_specs=[spec for _, spec in outs],
        scratch_shapes=scratch,
        compiler_params=pltpu.CompilerParams(
            collective_id=ident, has_side_effects=True, vmem_limit_bytes=limit << 20
        ),
        cost_estimate=pl.CostEstimate(flops=cost, bytes_accessed=1 << 24, transcendentals=0),
    )


def input_scratch():
    return [
        VM((T, 768), BF), VM((T, D), BF), VM((T, D), BF), VM((D, 384), BF), VM((D, 384), BF),
        DMA((9, NC)), DMA((9, NC)), DMA((2,)), DMA((2,)), DMA((3,)), DMA((NC,)), DMA((NC,)), DMA((NC,)),
    ]


def tail_scratch():
    def reduce(width):
        return [VM((T, width), BF), VM((2, T, 128), BF), VM((2, T, 128), BF), VM((2, T, B), BF), VM((2, T, B), BF)]

    pair = [DMA((2,)), DMA((2,))]
    return (
        [VM((2, T, B), BF), VM((512, 1024), BF), VM((T, B), BF), VM((T, D), BF), VM((D, 384), BF), VM((D, 384), BF)]
        + [VM((512, 1024), BF), VM((T, D), BF), VM((D, 1024), BF), VM((D, 1024), BF), VM((T, B), BF), VM((T, 768), F32)]
        + reduce(512) + reduce(512) + reduce(2048)
        + [DMA((5, NC))] * 6 + [DMA((9, NC))] * 4
        + pair * 5 + [DMA((8,)), DMA((3,)), DMA((8,)), DMA((1,)), DMA((8,))]
        + [DMA((16, NC)), DMA((16, NC)), DMA((NC,)), DMA((NC,)), DMA((NC,))]
    )


def per_device(latent, mod, *weights):
    (out,) = call(
        block, "block", 0, [ANY, INV] + [ANY] * 6, [((T, B), ANY)], input_scratch() + tail_scratch(), 63, 4 * 10**10
    )(latent.reshape(T, B), mod, *weights)
    return out.reshape(16, 64, B)


def solution(mesh):
    in_specs = (
        P("seq", None, "head"), P(), P(None, None, "head"), P("head", None),
        P(None, None, "head"), P("head", None), P(None, "head"), P("head", None),
    )
    return jax.shard_map(
        per_device, mesh=mesh, in_specs=in_specs, out_specs=P(None, "seq", "head"), check_vma=False
    )
```
